32 devices in a mesh: samp: 32 (over z, y, x, core).
Axes of the slice: x: 2, y: 2, z: 4, core: 2. Of those that a mesh axis runs over, the one named last changes fastest.
Arguments:
- inputs: float32 [30, 65536], P(None, 'samp'), may hold values from -1 to 1
- response: float32 [32, 65536], P(None, 'samp')
- multi_index: int32 [5456, 30], replicated, may hold values from 0 to 3, as said below
- chosen: int32 [3], replicated, may hold values from 0 to 5455, as said below
Outputs:
- residual: float32 [32, 65536], P(None, 'samp')
- correlations: float32 [3, 32, 5456], replicated
- coefficients: float32 [3, 32], replicated
The draws below stay inside these ranges and needn't reach their ends.
Inputs may be any that keep to these rules, and one draw needn't show every extreme that they name: `multi_index`: rows are distinct; each row's degrees sum to 3 or less. `chosen`: distinct indices.
All inputs are finite; a program needn't handle non-finite values. Where the reference program divides by a largest or mean magnitude, that divisor is 1e-20 or more.
Results may differ from the reference program's by a relative error of at most 0.0062.
Values sent between devices are 32-bit elements; how exact they have to be, the bound alone decides.
A program may use at most 128 MiB of HBM per device.

```python
import math
import jax
import jax.numpy as jnp
import numpy as np
from jax import lax

NVARS = 30
CANDS = 5456
RESP = 32
ITERS = 3
SAMPLES = 65536


def enumerate_table(count):
    rows = [[0] * count]
    for first in range(count):
        for degree in range(1, 4):
            row = [0] * count
            row[first] = degree
            rows.append(row)
    for first in range(count):
        for second in range(first + 1, count):
            for pair in ((1, 1), (2, 1), (1, 2)):
                row = [0] * count
                row[first] = pair[0]
                row[second] = pair[1]
                rows.append(row)
    for first in range(count):
        for second in range(first + 1, count):
            for third in range(second + 1, count):
                row = [0] * count
                row[first] = 1
                row[second] = 1
                row[third] = 1
                rows.append(row)
    return np.array(rows, dtype=np.int32)


def factor_table_drawn(inputs):
    x = inputs
    one = jnp.ones_like(x)
    second = (3.0 * x * x - 1.0) * 0.5
    third = (5.0 * x * x * x - 3.0 * x) * 0.5
    stacked = jnp.stack([one, x * math.sqrt(3.0), second * math.sqrt(5.0), third * math.sqrt(7.0)], axis=1)
    return stacked.reshape(x.shape[0] * 4, x.shape[1])


def slot_index_drawn(multi_index):
    count = multi_index.shape[1]
    positive = multi_index > 0
    rank = jnp.cumsum(positive.astype(jnp.int32), axis=1) - 1
    flat_pos = jnp.arange(count, dtype=jnp.int32)[None, :] * 4 + multi_index
    result = []
    for slot in range(3):
        picked = jnp.logical_and(positive, rank == slot)
        result.append(jnp.sum(jnp.where(picked, flat_pos, 0), axis=1).astype(jnp.int32))
    return tuple(result)


def draw_multi_index(key, part):
    table = jnp.asarray(enumerate_table(NVARS))
    order = jax.random.permutation(jax.random.fold_in(key, 11), CANDS)
    columns = jax.random.permutation(jax.random.fold_in(key, 12), NVARS)
    return table[order][:, columns].astype(jnp.int32)


def draw_chosen(key, part):
    middle = 1 + jax.random.permutation(jax.random.fold_in(key, 13), CANDS - 2)[:ITERS - 2]
    ends = jnp.array([0, CANDS - 1], dtype=jnp.int32)
    picks = jnp.concatenate([ends, middle.astype(jnp.int32)])
    order = jax.random.permutation(jax.random.fold_in(key, 19), ITERS)
    return picks[order].astype(jnp.int32)


def shared_data(key):
    uniform_x = jax.random.uniform(jax.random.fold_in(key, 14), (NVARS, SAMPLES), jnp.float32, -1.0, 1.0)
    inputs = uniform_x
    multi = draw_multi_index(key, 0)
    picks = draw_chosen(key, 0)
    flat = factor_table_drawn(inputs)
    index = slot_index_drawn(multi)
    active = jnp.take(flat, index[0][picks], axis=0) * jnp.take(flat, index[1][picks], axis=0) * jnp.take(flat, index[2][picks], axis=0)
    size = jax.random.uniform(jax.random.fold_in(key, 15), (ITERS, RESP), jnp.float32, 0.5, 2.0)
    flips = jax.random.randint(jax.random.fold_in(key, 16), (ITERS, RESP), 0, 2) * 2 - 1
    amps = size * flips.astype(jnp.float32)
    ramp = 1.0 + 2.0 * jnp.arange(SAMPLES, dtype=jnp.float32) / SAMPLES
    noise = jax.random.normal(jax.random.fold_in(key, 17), (RESP, SAMPLES), jnp.float32) * ramp * 0.5
    response = jnp.dot(amps.T, active, precision=jax.lax.Precision.HIGHEST) + noise
    return (inputs, response)


def draw_inputs(key, part):
    return shared_data(key)[0]


def draw_response(key, part):
    return shared_data(key)[1]


def setup_inputs(seed: int = 0) -> dict:
    arg_keys = jax.random.split(jax.random.key(seed), 5)
    inputs = draw_inputs(jax.random.fold_in(arg_keys[4], 71), 0)
    response = draw_response(jax.random.fold_in(arg_keys[4], 71), 0)
    multi_index = draw_multi_index(jax.random.fold_in(arg_keys[4], 71), 0)
    chosen = draw_chosen(jax.random.fold_in(arg_keys[4], 71), 0)
    return {"inputs": inputs, "response": response, "multi_index": multi_index, "chosen": chosen}


def factor_table(inputs):
    x = inputs
    one = jnp.ones_like(x)
    second = (3.0 * x * x - 1.0) * 0.5
    third = (5.0 * x * x * x - 3.0 * x) * 0.5
    stacked = jnp.stack([one, x * math.sqrt(3.0), second * math.sqrt(5.0), third * math.sqrt(7.0)], axis=1)
    return stacked.reshape(x.shape[0] * 4, x.shape[1])

def slot_index(multi_index):
    count = multi_index.shape[1]
    positive = multi_index > 0
    rank = jnp.cumsum(positive.astype(jnp.int32), axis=1) - 1
    flat_pos = jnp.arange(count, dtype=jnp.int32)[None, :] * 4 + multi_index
    result = []
    for slot in range(3):
        picked = jnp.logical_and(positive, rank == slot)
        result.append(lax.optimization_barrier(jnp.sum(jnp.where(picked, flat_pos, 0), axis=1)).astype(jnp.int32))
    return tuple(result)

def design(flat, index):
    first = jnp.take(flat, index[0], axis=0)
    second = jnp.take(flat, index[1], axis=0)
    third = jnp.take(flat, index[2], axis=0)
    return (first * second * third).astype(jnp.bfloat16)

def reference(inputs, response, multi_index, chosen):
    samples = inputs.shape[1]
    cands = multi_index.shape[0]
    iters = chosen.shape[0]
    resp = response.shape[0]
    flat = factor_table(inputs)
    index = slot_index(multi_index)
    active = design(flat, tuple((i[chosen] for i in index)))
    gram = jnp.dot(active.astype(jnp.float32), active.T.astype(jnp.float32), preferred_element_type=jnp.float32)
    width = math.gcd(samples, 4096)
    nblocks = samples // width

    def correlate(rb):

        def step(i, acc):
            piece = lax.dynamic_slice_in_dim(flat, i * width, width, 1)
            part = lax.dynamic_slice_in_dim(rb, i * width, width, 1)
            psi = design(piece, index)
            return acc + lax.dot_general(part.astype(jnp.float32), psi.astype(jnp.float32), (((1,), (1,)), ((), ())), preferred_element_type=jnp.float32)
        return lax.fori_loop(0, nblocks, step, jnp.zeros((resp, cands), jnp.float32))
    residual = response
    coefs = jnp.zeros((iters, resp), jnp.float32)
    outs = []
    for k in range(iters):
        rb = residual.astype(jnp.bfloat16)
        corr = correlate(rb)
        sq = lax.optimization_barrier(jnp.sum(residual * residual, axis=1))
        norm = math.sqrt(samples) * jnp.sqrt(sq / samples + 1e-06)
        outs.append(corr / norm[:, None])
        largest = lax.optimization_barrier(jnp.max(jnp.abs(corr), axis=1))
        gamma = jnp.abs(corr[:, chosen[k]]) / (largest + 1e-06)
        factor = jnp.linalg.cholesky(gram[:k + 1, :k + 1])
        target = corr[:, chosen[:k + 1]].T
        weights = jax.scipy.linalg.cho_solve((factor, True), target)
        update = jnp.dot(weights.T, active[:k + 1].astype(jnp.float32), precision=lax.Precision.HIGHEST)
        residual = residual - gamma[:, None] * update
        coefs = coefs.at[:k + 1].add(weights * gamma[None, :])
    return (residual, jnp.stack(outs), coefs)
```

```python
import functools
import math

import jax
import jax.numpy as jnp
from jax import lax
from jax.experimental import pallas as pl
from jax.experimental.pallas import tpu as pltpu
from jax.sharding import PartitionSpec as P

LANES = 128
NT = (((1,), (1,)), ((), ()))
TN = (((0,), (0,)), ((), ()))
MESH = pl.DeviceIdType.MESH
VMEM_LIMIT = 56 * 2**20


def up(n, m):
    return -(-n // m) * m


def split(x):
    high = x.astype(jnp.bfloat16)
    return high, (x - high.astype(jnp.float32)).astype(jnp.bfloat16)


class Basis:
    def __init__(self, nvars):
        self.nvars = nvars
        self.stride = up(nvars + 1, 16)
        gaps = []
        d = 1
        while nvars - 3 * d > 0:
            gaps += [(d, e) for e in range(d, nvars - 2 * d)]
            d += 1
        if nvars % 3 == 0:
            gaps.append((nvars // 3, nvars // 3))
        self.triples = len(gaps)
        self.pairs = nvars // 2
        self.squares = nvars - 1
        self.blocks = [("triple", d, d + e) for d, e in gaps]
        self.blocks += [("pair", d, 0) for d in range(1, self.pairs + 1)]
        self.blocks += [("square", d, 0) for d in range(1, self.squares + 1)]
        self.blocks += [("single", e, 0) for e in range(3)]
        while len(self.blocks) * self.stride % LANES:
            self.blocks.append(("single", 0, 0))
        self.lines = len(self.blocks) * self.stride // LANES
        self.height = up(self.lines + 1, 24)


def place(multi, basis):
    n = float(basis.nvars)
    deg = multi.astype(jnp.float32)
    var = lax.broadcasted_iota(jnp.int32, multi.shape, 0).astype(jnp.float32)
    pos = deg > 0.0
    down = lambda f, x: f(x, axis=0, keepdims=True)
    count = down(jnp.sum, jnp.where(pos, 1.0, 0.0))
    total = down(jnp.sum, jnp.where(pos, var, 0.0))
    low = down(jnp.min, jnp.where(pos, var, n))
    high = down(jnp.max, jnp.where(pos, var, 0.0))
    most = down(jnp.max, deg)
    two = down(jnp.sum, jnp.where(deg > 1.5, var, 0.0))
    mid = total - low - high
    g1, g2 = mid - low, high - mid
    g3 = n - g1 - g2
    at_mid = jnp.logical_and(g2 <= g3, g2 < g1)
    at_high = jnp.logical_and(g3 <= g1, g3 < g2)
    pick = lambda a, b, c: jnp.where(at_high, c, jnp.where(at_mid, b, a))
    d1, d2, start3 = pick(g1, g2, g3), pick(g2, g3, g1), pick(low, mid, high)
    block3 = n * (d1 - 1.0) - 1.5 * d1 * (d1 - 1.0) + d2 - d1
    gap = high - low
    near = gap <= n - gap
    block2 = float(basis.triples - 1) + jnp.where(near, gap, n - gap)
    start2 = jnp.where(near, low, high)
    one = total - two
    turn = two - one
    block21 = float(basis.triples + basis.pairs - 1) + jnp.where(turn > 0.0, turn, turn + n)
    base = float(basis.triples + basis.pairs + basis.squares)
    block1 = base + jnp.maximum(most - 1.0, 0.0)
    squared = most > 1.5
    block = jnp.where(
        count > 2.5, block3, jnp.where(count > 1.5, jnp.where(squared, block21, block2), block1)
    )
    start = jnp.where(
        count > 2.5, start3, jnp.where(count > 1.5, jnp.where(squared, one, start2), low)
    )
    index = block * float(basis.stride) + start
    line = jnp.floor(index * (1.0 / LANES))
    return line, index - line * float(LANES)


def correlate(basis, iters, deep, chosen_ref, x_ref, res_ref, multi_ref, out_ref, active_ref, twice, turned, rows, acc):
    nvars, width = x_ref.shape
    resp = res_ref.shape[0]
    stride = basis.stride
    few = active_ref.shape[0]
    x = x_ref[...]
    second = (3.0 * x * x - 1.0) * 0.5
    third = (5.0 * x * x * x - 3.0 * x) * 0.5
    values = [x * math.sqrt(3.0), second * math.sqrt(5.0), third * math.sqrt(7.0)]
    tall = twice.shape[0] // 3
    for e, value in enumerate(values):
        twice[e * tall : (e + 1) * tall, :] = jnp.ones((tall, width), jnp.float32)
        twice[e * tall : e * tall + nvars, :] = value
    for d in range(nvars):
        if d:
            turned[d * stride : d * stride + nvars - d, :] = values[0][d:]
            turned[d * stride + nvars - d : d * stride + nvars, :] = values[0][:d]
            turned[(nvars + d) * stride : (nvars + d) * stride + nvars - d, :] = values[1][d:]
            turned[(nvars + d) * stride + nvars - d : (nvars + d) * stride + nvars, :] = values[1][:d]
    zero = jnp.zeros((stride - nvars, width), jnp.float32)
    for d in range(1, nvars):
        turned[d * stride + nvars : (d + 1) * stride, :] = zero
        turned[(nvars + d) * stride + nvars : (nvars + d + 1) * stride, :] = zero

    high, low = split(res_ref[...])
    rows[0:resp, :] = high
    rows[resp : 2 * resp, :] = low
    multi = multi_ref[...]
    column = lax.broadcasted_iota(jnp.int32, multi.shape, 1)
    line = lax.broadcasted_iota(jnp.int32, (few, width), 0)
    actives = jnp.zeros((few, width), jnp.float32)
    for k in range(iters):
        deg = jnp.sum(
            jnp.where(column == chosen_ref[k], multi, 0).astype(jnp.float32), axis=1, keepdims=True
        )
        v = jnp.where(
            deg > 2.5,
            values[2],
            jnp.where(deg > 1.5, values[1], jnp.where(deg > 0.5, values[0], 1.0)),
        )
        p = v[0:8]
        for i in range(8, nvars - 7, 8):
            p = p * v[i : i + 8]
        row = p[0:1]
        for i in range(1, min(8, nvars)):
            row = row * p[i : i + 1]
        for i in range(nvars // 8 * 8, nvars):
            row = row * v[i : i + 1]
        actives = jnp.where(line == k, row, actives)
    actives = actives.astype(jnp.bfloat16)
    active_ref[...] = actives
    rows[2 * resp : 2 * resp + few, :] = actives
    rest = rows.shape[0] - 2 * resp - few
    rows[2 * resp + few :, :] = jnp.zeros((rest, width), jnp.bfloat16)

    per = 512 // stride
    groups = [basis.blocks[i : i + per] for i in range(0, len(basis.blocks), per)]

    def step(k, first):
        for g, group in enumerate(groups):
            total = None
            for half in range(0, deep, 256):
                cols = pl.ds(pl.multiple_of(k * deep + half, 256), 256)
                f1 = twice[0:stride, cols]
                parts = []
                held = None
                for kind, d, e in group:
                    if kind == "triple":
                        if held != d:
                            pair = f1 * turned[d * stride : (d + 1) * stride, cols]
                            held = d
                        part = pair * turned[e * stride : (e + 1) * stride, cols]
                    elif kind == "pair":
                        part = f1 * turned[d * stride : (d + 1) * stride, cols]
                    elif kind == "square":
                        part = f1 * turned[(nvars + d) * stride : (nvars + d + 1) * stride, cols]
                    else:
                        part = twice[d * tall : d * tall + stride, cols]
                    parts.append(part.astype(jnp.bfloat16))
                psi = jnp.concatenate(parts, axis=0)
                term = lax.dot_general(psi, rows[:, cols], NT, preferred_element_type=jnp.float32)
                total = term if total is None else total + term
            span = slice(g * per * stride, (g * per + len(group)) * stride)
            acc[span, :] = total if first else acc[span, :] + total

    step(0, True)

    @pl.loop(1, width // deep)
    def _(k):
        step(k, False)

    height = basis.height
    for b in range(basis.lines):
        t = acc[b * LANES : (b + 1) * LANES, :].T
        corr = t[0:resp] + t[resp : 2 * resp]
        for q in range(0, resp, 8):
            out_ref[pl.ds(q * height + b, 8, stride=height), :] = corr[q : q + 8]
        out_ref[pl.ds(resp * height + b, 8, stride=height), :] = t[2 * resp : 2 * resp + 8]
    res = res_ref[...]
    sq = jnp.broadcast_to(jnp.sum(res * res, axis=1, keepdims=True), (resp, LANES))
    for b in range(basis.lines, height):
        for q in range(0, resp, 8):
            out_ref[pl.ds(q * height + b, 8, stride=height), :] = sq[q : q + 8]
        out_ref[pl.ds(resp * height + b, 8, stride=height), :] = jnp.zeros((8, LANES), jnp.float32)


def radices(n):
    result, stride = [], 1
    while n > 1:
        r = 2 if stride == 1 or n == 2 else 4
        if n % r:
            raise ValueError("device count")
        result.append((r, stride))
        stride *= r
        n //= r
    return result


def halving(count, stages):
    plan = []
    for r, _ in stages:
        cut = count % r == 0
        count = count // r if cut else count
        plan.append((cut, count))
    return plan


class Semaphores:
    def __init__(self, send, recv):
        self.send, self.recv, self.used, self.sent = send, recv, 0, []

    def copy(self, src, dst, peer):
        c = pltpu.make_async_remote_copy(
            src_ref=src,
            dst_ref=dst,
            send_sem=self.send.at[self.used],
            recv_sem=self.recv.at[self.used],
            device_id=(peer,),
            device_id_type=MESH,
        )
        self.used += 1
        self.sent.append(c)
        c.start()
        return c


class Stream:
    def __init__(self, ctx, part, lines, offset, held, landed):
        self.ctx, self.lines = ctx, lines
        self.now = (part, offset)
        self.held, self.landed = held, landed
        self.plan = halving(ctx["counts"][id(part)], ctx["stages"])
        self.waiting = None

    def send(self, s):
        r, stride = self.ctx["stages"][s]
        digit = self.ctx["digits"][s]
        cut, count = self.plan[s]
        src, base = self.now
        copies = []
        for j in range(1, r):
            other = lax.rem(digit + j, r)
            peer = self.ctx["me"] + (other - digit) * stride
            at = base + other * count if cut else base
            copies.append(
                self.ctx["sems"].copy(
                    src.at[pl.ds(at, count), self.lines],
                    self.landed[s].at[j, :, self.lines],
                    peer,
                )
            )
        self.waiting = copies

    def receive(self, s):
        r, _ = self.ctx["stages"][s]
        digit = self.ctx["digits"][s]
        cut, count = self.plan[s]
        src, base = self.now
        for c in self.waiting:
            c.wait_recv()
        at = base + digit * count if cut else base
        own = src[pl.ds(at, count), self.lines]
        landed = self.landed[s]
        if cut:
            total = own
            for j in range(1, r):
                total = total + landed[j, :, self.lines]
        else:
            landed[0, :, self.lines] = own
            total = landed[pl.ds(digit, 1), :, self.lines][0]
            for i in range(1, r):
                total = total + landed[pl.ds(lax.rem(digit + r - i, r), 1), :, self.lines][0]
        self.held[s][:, self.lines] = total
        self.now = (self.held[s], 0)


def spread(ctx, plan, whole):
    levels = [s for s, (cut, _) in enumerate(plan) if cut]
    size = plan[-1][1]

    def where(digits):
        at, weight = 0, size
        for s in reversed(levels):
            at = at + digits[s] * weight
            weight *= ctx["stages"][s][0]
        return at

    own = {s: ctx["digits"][s] for s in levels}
    arriving = {s: [] for s in levels}

    def forward(digits, below):
        for s in reversed(below):
            r, stride = ctx["stages"][s]
            digit = ctx["digits"][s]
            for j in range(1, r):
                peer = ctx["me"] + (lax.rem(digit + j, r) - digit) * stride
                block = whole.at[pl.ds(where(digits), size)]
                c = ctx["sems"].copy(block, block, peer)
                source = dict(digits)
                source[s] = lax.rem(digit + r - j, r)
                arriving[s].append((c, source))

    def run():
        for i in reversed(range(len(levels))):
            for c, digits in arriving[levels[i]]:
                c.wait_recv()
                forward(digits, levels[:i])

    forward(own, levels)
    return where(own), run


def exchange(basis, devices, parts, iters, halves, part_ref, gram_ref, multi_ref, out_ref, *scratch):
    scratch = list(scratch)
    resp, height = part_ref.shape[0], basis.height
    cands = multi_ref.shape[1]
    stages = radices(devices)
    me = lax.axis_index("samp")
    digits = [lax.rem(me // stride, r) for r, stride in stages]
    send, recv, total, gram, maps, hot = scratch[:6]
    buffers = scratch[6:]
    k = len(stages)
    held, landed, gheld, glanded = (buffers[i * k : (i + 1) * k] for i in range(4))

    barrier = pltpu.get_barrier_semaphore()
    peers = 0
    for (r, stride), digit in zip(stages, digits):
        for j in range(1, r):
            peer = me + (lax.rem(digit + j, r) - digit) * stride
            pl.semaphore_signal(barrier, inc=1, device_id=(peer,), device_id_type=MESH)
            peers += 1
    pl.semaphore_wait(barrier, peers)

    ctx = {
        "me": me,
        "digits": digits,
        "stages": stages,
        "sems": Semaphores(send, recv),
        "counts": {id(part_ref): resp, id(gram_ref): gram_ref.shape[0]},
    }
    high = height // parts
    grams = Stream(ctx, gram_ref, slice(0, gram_ref.shape[1]), 0, gheld, glanded)
    streams = [grams] + [
        Stream(ctx, part_ref, slice(p * high, (p + 1) * high), 0, held, landed) for p in range(parts)
    ]
    for s in streams:
        s.send(0)

    line, lane = place(multi_ref[...], basis)
    maps[...] = jnp.zeros_like(maps)
    maps[0:1, 0:cands] = line
    maps[1:2, 0:cands] = lane
    for c in range(0, maps.shape[1], LANES):
        at = maps[0:1, c : c + LANES]
        row = lax.broadcasted_iota(jnp.int32, (height, LANES), 0).astype(jnp.float32)
        one = jnp.where(row == at, 1.0, 0.0).astype(jnp.bfloat16)
        for i in range(3):
            hot[i * height : (i + 1) * height, c : c + LANES] = one

    for stage in range(k):
        for s in streams:
            s.receive(stage)
            if stage + 1 < k:
                s.send(stage + 1)

    def arrange(row, store):
        first, rest = split(row)
        _, third = split(row - first.astype(jnp.float32))
        stacked = jnp.concatenate([first, rest, third], axis=0)
        wide = 4 * LANES
        for c in range(0, maps.shape[1], wide):
            size = min(wide, maps.shape[1] - c)
            found = lax.dot_general(
                stacked, hot[:, c : c + size], TN, preferred_element_type=jnp.float32
            )
            for i in range(0, size, LANES):
                at = maps[1:2, c + i : c + i + LANES]
                lo = lax.broadcasted_iota(jnp.int32, (LANES, LANES), 0).astype(jnp.float32)
                kept = jnp.where(lo == at, found[:, i : i + LANES], 0.0)
                store((c + i) // LANES, jnp.sum(kept, axis=0, keepdims=True))

    gplan, plan = grams.plan, streams[1].plan
    last, _ = grams.now
    gdigits = [s for s, (cut, _) in enumerate(gplan) if cut]
    at, weight = 0, gplan[-1][1]
    for s in reversed(gdigits):
        at = at + digits[s] * weight
        weight *= stages[s][0]
    gram[pl.ds(at, gplan[-1][1])] = last[...]
    _, run_gram = spread(ctx, gplan, gram)

    count = plan[-1][1]
    at, weight = 0, count
    for s in reversed([s for s, (cut, _) in enumerate(plan) if cut]):
        at = at + digits[s] * weight
        weight *= stages[s][0]
    reduced = held[-1]
    for i in range(count):
        row = reduced[i]
        total[pl.ds(at + i, 1)] = row[None]

        def store(b, value, i=i):
            total[pl.ds(at + i, 1), b : b + 1, :] = value[None]

        arrange(row, store)
    _, run = spread(ctx, plan, total)
    run_gram()
    for g in range(iters):
        row = jnp.concatenate([gram[g * halves + h] for h in range(halves)], axis=0)

        def store(b, value, g=g):
            out_ref[resp + g, b : b + 1, :] = value

        out_ref[resp + g] = row
        arrange(row, store)
    run()
    for g in range(iters, out_ref.shape[0] - resp):
        out_ref[resp + g] = jnp.zeros((height, LANES), jnp.float32)
    out_ref[0:resp] = total[...]
    for c in ctx["sems"].sent:
        c.wait_send()


def finish(cands, samples, iters, height, chosen_ref, total_ref, res_ref, active_ref, out_ref, corr_ref, coef_ref, flat):
    resp = res_ref.shape[0]
    for b in range(flat.shape[1] // LANES):
        for q in range(0, flat.shape[0], 8):
            flat[q : q + 8, b * LANES : (b + 1) * LANES] = total_ref[
                pl.ds(q * height + b, 8, stride=height), :
            ]
    sq = jnp.concatenate(
        [total_ref[pl.ds(q * height + height - 1, 8, stride=height), :] for q in range(0, resp, 8)],
        axis=0,
    )[:, 0:1]
    total = flat[:, 0:cands]
    column = lax.broadcasted_iota(jnp.int32, total.shape, 1)
    picked = [
        jnp.sum(jnp.where(column == chosen_ref[i], total, 0.0), axis=1, keepdims=True)
        for i in range(iters)
    ]
    target = [p[0:resp] for p in picked]
    gram = [[picked[j][resp + i : resp + i + 1] for j in range(iters)] for i in range(iters)]
    tri = [[None] * iters for _ in range(iters)]
    for i in range(iters):
        for j in range(i + 1):
            s = gram[i][j]
            for m in range(j):
                s = s - tri[i][m] * tri[j][m]
            tri[i][j] = jnp.sqrt(s) if i == j else s / tri[j][j]
    corr = total[0:resp]
    rows = [total[resp + i : resp + i + 1] for i in range(iters)]
    coef = [jnp.zeros((resp, 1), jnp.float32) for _ in range(iters)]
    for k in range(iters):
        norm = math.sqrt(samples) * jnp.sqrt(sq / samples + 1e-06)
        corr_ref[k] = corr * (1.0 / norm)
        largest = jnp.max(jnp.abs(corr), axis=1, keepdims=True)
        gamma = jnp.abs(target[k]) / (largest + 1e-06)
        w = []
        for i in range(k + 1):
            s = target[i]
            for m in range(i):
                s = s - tri[i][m] * w[m]
            w.append(s / tri[i][i])
        for i in reversed(range(k + 1)):
            s = w[i]
            for m in range(i + 1, k + 1):
                s = s - tri[m][i] * w[m]
            w[i] = s / tri[i][i]
        step = [gamma * wi for wi in w]
        for i in range(k + 1):
            coef[i] = coef[i] + step[i]
        if k < iters - 1:
            gain = sum(wi * t for wi, t in zip(w, target))
            sq = jnp.maximum(sq - gamma * (2.0 - gamma) * gain, 0.0)
            target = [
                target[j] - sum(step[i] * gram[i][j] for i in range(k + 1)) for j in range(iters)
            ]
            for i in range(k + 1):
                corr = corr - step[i] * rows[i]
    res = res_ref[...]
    active = active_ref[...].astype(jnp.float32)
    for i in range(iters):
        res = res - coef[i] * active[i : i + 1]
    out_ref[...] = res
    shape = (resp, resp)
    eye = lax.broadcasted_iota(jnp.int32, shape, 0) == lax.broadcasted_iota(jnp.int32, shape, 1)
    lines = [jnp.sum(jnp.where(eye, c, 0.0), axis=0, keepdims=True) for c in coef]
    line = lax.broadcasted_iota(jnp.int32, coef_ref.shape, 0)
    coef_ref[...] = sum(jnp.where(line == i, lines[i], 0.0) for i in range(iters))


def on_device(inputs, response, multi_index, chosen):
    nvars, width = inputs.shape
    devices = lax.axis_size("samp")
    samples = width * devices
    cands = multi_index.shape[0]
    iters = chosen.shape[0]
    resp = response.shape[0]
    basis = Basis(nvars)
    height, stride = basis.height, basis.stride
    few = up(iters, 16)
    kept = up(iters, 4)
    extra = up(kept, 8)
    used = resp + extra
    multi = multi_index.T
    vmem = pl.BlockSpec(memory_space=pltpu.VMEM)
    smem = pl.BlockSpec(memory_space=pltpu.SMEM)
    deep = math.gcd(width, 512)
    local, active = pl.pallas_call(
        functools.partial(correlate, basis, iters, deep),
        in_specs=[smem, vmem, vmem, vmem],
        out_specs=[vmem, vmem],
        out_shape=[
            jax.ShapeDtypeStruct((used * height, LANES), jnp.float32),
            jax.ShapeDtypeStruct((few, width), jnp.bfloat16),
        ],
        scratch_shapes=[
            pltpu.VMEM((3 * stride, width), jnp.float32),
            pltpu.VMEM((2 * nvars * stride, width), jnp.float32),
            pltpu.VMEM((up(2 * resp + few, LANES), width), jnp.bfloat16),
            pltpu.VMEM((basis.lines * LANES, LANES), jnp.float32),
        ],
        compiler_params=pltpu.CompilerParams(vmem_limit_bytes=VMEM_LIMIT),
        name="correlate",
    )(chosen, inputs, response, multi)

    halves = 2
    part = local[: resp * height].reshape(resp, height, LANES)
    gram = local[resp * height : (resp + kept) * height]
    gram = gram.reshape(kept * halves, height // halves, LANES)
    stages = radices(devices)
    parts = 2
    plan, gplan = halving(resp, stages), halving(gram.shape[0], stages)
    copies = (parts + 1) * sum(r - 1 for r, _ in stages)
    copies += resp // plan[-1][1] + gram.shape[0] // gplan[-1][1] - 2
    grid = up(cands, LANES)
    held = [pltpu.VMEM((c, height, LANES), jnp.float32) for _, c in plan]
    landed = [pltpu.VMEM((r, c, height, LANES), jnp.float32) for (r, _), (_, c) in zip(stages, plan)]
    unit = gram.shape[1:]
    gheld = [pltpu.VMEM((c, *unit), jnp.float32) for _, c in gplan]
    glanded = [pltpu.VMEM((r, c, *unit), jnp.float32) for (r, _), (_, c) in zip(stages, gplan)]
    total = pl.pallas_call(
        functools.partial(exchange, basis, devices, parts, iters, halves),
        in_specs=[vmem, vmem, vmem],
        out_specs=vmem,
        out_shape=jax.ShapeDtypeStruct((used, height, LANES), jnp.float32),
        scratch_shapes=[
            pltpu.SemaphoreType.DMA((copies,)),
            pltpu.SemaphoreType.DMA((copies,)),
            pltpu.VMEM((resp, height, LANES), jnp.float32),
            pltpu.VMEM(gram.shape, jnp.float32),
            pltpu.VMEM((8, grid), jnp.float32),
            pltpu.VMEM((3 * height, grid), jnp.bfloat16),
            *held,
            *landed,
            *gheld,
            *glanded,
        ],
        compiler_params=pltpu.CompilerParams(
            vmem_limit_bytes=VMEM_LIMIT, collective_id=0, has_side_effects=True
        ),
        name="exchange",
    )(part, gram, multi)
    residual, corr, coef = pl.pallas_call(
        functools.partial(finish, cands, samples, iters, height),
        in_specs=[smem, vmem, vmem, vmem],
        out_specs=[vmem, vmem, vmem],
        out_shape=[
            jax.ShapeDtypeStruct((resp, width), jnp.float32),
            jax.ShapeDtypeStruct((iters, resp, cands), jnp.float32),
            jax.ShapeDtypeStruct((extra, resp), jnp.float32),
        ],
        scratch_shapes=[pltpu.VMEM((used, grid), jnp.float32)],
        compiler_params=pltpu.CompilerParams(vmem_limit_bytes=VMEM_LIMIT),
        name="finish",
    )(chosen, total.reshape(used * height, LANES), response, active)
    return residual, corr, coef[:iters]


def solution(mesh):
    placed = (P(None, "samp"), P(None, "samp"), P(), P())
    return jax.shard_map(
        on_device,
        mesh=mesh,
        in_specs=placed,
        out_specs=(P(None, "samp"), P(), P()),
        check_vma=False,
    )
```

```python
import functools
import math

import jax
import jax.numpy as jnp
from jax import lax
from jax.experimental import pallas as pl
from jax.experimental.pallas import tpu as pltpu
from jax.sharding import PartitionSpec as P

LANES = 128
NT = (((1,), (1,)), ((), ()))
TN = (((0,), (0,)), ((), ()))
MESH = pl.DeviceIdType.MESH
VMEM_LIMIT = 56 * 2**20


def up(n, m):
    return -(-n // m) * m


def split(x):
    high = x.astype(jnp.bfloat16)
    return high, (x - high.astype(jnp.float32)).astype(jnp.bfloat16)


class Basis:
    def __init__(self, nvars):
        self.nvars = nvars
        self.stride = up(nvars + 1, 16)
        gaps = []
        d = 1
        while nvars - 3 * d > 0:
            gaps += [(d, e) for e in range(d, nvars - 2 * d)]
            d += 1
        if nvars % 3 == 0:
            gaps.append((nvars // 3, nvars // 3))
        self.triples = len(gaps)
        self.pairs = nvars // 2
        self.squares = nvars - 1
        self.blocks = [("triple", d, d + e) for d, e in gaps]
        self.blocks += [("pair", d, 0) for d in range(1, self.pairs + 1)]
        self.blocks += [("square", d, 0) for d in range(1, self.squares + 1)]
        self.blocks += [("single", e, 0) for e in range(3)]
        while len(self.blocks) * self.stride % LANES:
            self.blocks.append(("single", 0, 0))
        self.lines = len(self.blocks) * self.stride // LANES
        self.height = up(self.lines + 1, 24)


def place(multi, basis):
    n = float(basis.nvars)
    deg = multi.astype(jnp.float32)
    var = lax.broadcasted_iota(jnp.int32, multi.shape, 0).astype(jnp.float32)
    pos = deg > 0.0
    down = lambda f, x: f(x, axis=0, keepdims=True)
    count = down(jnp.sum, jnp.where(pos, 1.0, 0.0))
    total = down(jnp.sum, jnp.where(pos, var, 0.0))
    low = down(jnp.min, jnp.where(pos, var, n))
    high = down(jnp.max, jnp.where(pos, var, 0.0))
    most = down(jnp.max, deg)
    two = down(jnp.sum, jnp.where(deg > 1.5, var, 0.0))
    mid = total - low - high
    g1, g2 = mid - low, high - mid
    g3 = n - g1 - g2
    at_mid = jnp.logical_and(g2 <= g3, g2 < g1)
    at_high = jnp.logical_and(g3 <= g1, g3 < g2)
    pick = lambda a, b, c: jnp.where(at_high, c, jnp.where(at_mid, b, a))
    d1, d2, start3 = pick(g1, g2, g3), pick(g2, g3, g1), pick(low, mid, high)
    block3 = n * (d1 - 1.0) - 1.5 * d1 * (d1 - 1.0) + d2 - d1
    gap = high - low
    near = gap <= n - gap
    block2 = float(basis.triples - 1) + jnp.where(near, gap, n - gap)
    start2 = jnp.where(near, low, high)
    one = total - two
    turn = two - one
    block21 = float(basis.triples + basis.pairs - 1) + jnp.where(turn > 0.0, turn, turn + n)
    base = float(basis.triples + basis.pairs + basis.squares)
    block1 = base + jnp.maximum(most - 1.0, 0.0)
    squared = most > 1.5
    block = jnp.where(
        count > 2.5, block3, jnp.where(count > 1.5, jnp.where(squared, block21, block2), block1)
    )
    start = jnp.where(
        count > 2.5, start3, jnp.where(count > 1.5, jnp.where(squared, one, start2), low)
    )
    index = block * float(basis.stride) + start
    line = jnp.floor(index * (1.0 / LANES))
    return line, index - line * float(LANES)


def prepare(basis, iters, chosen_ref, x_ref, res_ref, multi_ref, active_ref, twice, turned, rows):
    nvars, width = x_ref.shape
    resp = res_ref.shape[0]
    stride = basis.stride
    few = active_ref.shape[0]
    x = x_ref[...]
    second = (3.0 * x * x - 1.0) * 0.5
    third = (5.0 * x * x * x - 3.0 * x) * 0.5
    values = [x * math.sqrt(3.0), second * math.sqrt(5.0), third * math.sqrt(7.0)]
    for e, value in enumerate(values):
        twice[e * stride + nvars : (e + 1) * stride, :] = jnp.ones((stride - nvars, width), jnp.float32)
        twice[e * stride : e * stride + nvars, :] = value
    zero = jnp.zeros((stride - nvars, width), jnp.float32)
    for e in range(2):
        for d in range(1, nvars):
            at = (e * nvars + d) * stride
            turned[at : at + nvars - d, :] = values[e][d:]
            turned[at + nvars - d : at + nvars, :] = values[e][:d]
            turned[at + nvars : at + stride, :] = zero

    high, low = split(res_ref[...])
    rows[0:resp, :] = high
    rows[resp : 2 * resp, :] = low
    multi = multi_ref[...]
    column = lax.broadcasted_iota(jnp.int32, multi.shape, 1)
    line = lax.broadcasted_iota(jnp.int32, (few, width), 0)
    actives = jnp.zeros((few, width), jnp.float32)
    for k in range(iters):
        deg = jnp.sum(
            jnp.where(column == chosen_ref[k], multi, 0).astype(jnp.float32), axis=1, keepdims=True
        )
        v = jnp.where(
            deg > 2.5,
            values[2],
            jnp.where(deg > 1.5, values[1], jnp.where(deg > 0.5, values[0], 1.0)),
        )
        p = v[0:8]
        for i in range(8, nvars - 7, 8):
            p = p * v[i : i + 8]
        row = p[0:1]
        for i in range(1, min(8, nvars)):
            row = row * p[i : i + 1]
        for i in range(nvars // 8 * 8, nvars):
            row = row * v[i : i + 1]
        actives = jnp.where(line == k, row, actives)
    actives = actives.astype(jnp.bfloat16)
    active_ref[...] = actives
    rows[2 * resp : 2 * resp + few, :] = actives
    rest = rows.shape[0] - 2 * resp - few
    rows[2 * resp + few :, :] = jnp.zeros((rest, width), jnp.bfloat16)


def correlate(basis, blocks, deep, twice, turned, rows, acc):
    stride, nvars = basis.stride, basis.nvars
    width = rows.shape[1]
    per = 512 // stride
    groups = [blocks[i : i + per] for i in range(0, len(blocks), per)]

    def step(k, first):
        for g, group in enumerate(groups):
            total = None
            for half in range(0, deep, 256):
                at = k * deep + half
                cols = pl.ds(at if first else pl.multiple_of(at, 256), 256)
                f1 = twice[0:stride, cols]
                parts = []
                held = None
                for kind, d, e in group:
                    if kind == "triple":
                        if held != d:
                            pair = f1 * turned[d * stride : (d + 1) * stride, cols]
                            held = d
                        part = pair * turned[e * stride : (e + 1) * stride, cols]
                    elif kind == "pair":
                        part = f1 * turned[d * stride : (d + 1) * stride, cols]
                    elif kind == "square":
                        part = f1 * turned[(nvars + d) * stride : (nvars + d + 1) * stride, cols]
                    else:
                        part = twice[d * stride : (d + 1) * stride, cols]
                    parts.append(part.astype(jnp.bfloat16))
                psi = jnp.concatenate(parts, axis=0)
                term = lax.dot_general(psi, rows[:, cols], NT, preferred_element_type=jnp.float32)
                total = term if total is None else total + term
            span = slice(g * per * stride, (g * per + len(group)) * stride)
            acc[span, :] = total if first else acc[span, :] + total

    step(0, True)

    if width > deep:

        @pl.loop(1, width // deep)
        def _(k):
            step(k, False)


def radices(n):
    result, stride = [], 1
    while n > 1:
        r = 2 if stride == 1 or n == 2 else 4
        if n % r:
            raise ValueError("device count")
        result.append((r, stride))
        stride *= r
        n //= r
    return result


def halving(count, stages):
    plan = []
    for r, _ in stages:
        cut = count % r == 0
        count = count // r if cut else count
        plan.append((cut, count))
    return plan


class Semaphores:
    def __init__(self, send, recv):
        self.send, self.recv, self.used, self.sent = send, recv, 0, []

    def copy(self, src, dst, peer):
        c = pltpu.make_async_remote_copy(
            src_ref=src,
            dst_ref=dst,
            send_sem=self.send.at[self.used],
            recv_sem=self.recv.at[self.used],
            device_id=(peer,),
            device_id_type=MESH,
        )
        self.used += 1
        self.sent.append(c)
        c.start()
        return c


class Stream:
    def __init__(self, ctx, part, count, unit, held, landed):
        self.ctx, self.unit = ctx, unit
        self.now = part
        self.held, self.landed = held, landed
        self.plan = halving(count, ctx["stages"])
        self.waiting = None

    def send(self, s):
        r, stride = self.ctx["stages"][s]
        digit = self.ctx["digits"][s]
        cut, count = self.plan[s]
        size = count * self.unit
        copies = []
        for j in range(1, r):
            other = lax.rem(digit + j, r)
            peer = self.ctx["me"] + (other - digit) * stride
            at = pl.multiple_of(other * size, 8) if cut else 0
            copies.append(
                self.ctx["sems"].copy(
                    self.now.at[pl.ds(at, size)], self.landed[s].at[pl.ds(j * size, size)], peer
                )
            )
        self.waiting = copies

    def receive(self, s):
        r, _ = self.ctx["stages"][s]
        digit = self.ctx["digits"][s]
        cut, count = self.plan[s]
        size = count * self.unit
        for c in self.waiting:
            c.wait_recv()
        at = pl.multiple_of(digit * size, 8) if cut else 0
        own = self.now[pl.ds(at, size), :]
        landed = self.landed[s]
        if cut:
            total = own
            for j in range(1, r):
                total = total + landed[j * size : (j + 1) * size, :]
        else:
            landed[0:size, :] = own
            total = None
            for i in range(r):
                at = pl.multiple_of(lax.rem(digit + r - i, r) * size, 8)
                term = landed[pl.ds(at, size), :]
                total = term if total is None else total + term
        self.held[s][...] = total
        self.now = self.held[s]


def digit_place(ctx, plan, digits):
    at, weight = 0, plan[-1][1]
    for s in reversed(range(len(plan))):
        if plan[s][0]:
            at = at + digits[s] * weight
            weight *= ctx["stages"][s][0]
    return at


def spread(ctx, plan, unit, whole):
    levels = [s for s, (cut, _) in enumerate(plan) if cut]
    size = plan[-1][1] * unit
    arriving = {s: [] for s in levels}

    def forward(digits, below):
        at = pl.multiple_of(digit_place(ctx, plan, digits) * unit, 8)
        block = whole.at[pl.ds(at, size)]
        for s in reversed(below):
            r, stride = ctx["stages"][s]
            digit = ctx["digits"][s]
            for j in range(1, r):
                peer = ctx["me"] + (lax.rem(digit + j, r) - digit) * stride
                c = ctx["sems"].copy(block, block, peer)
                source = dict(digits)
                source[s] = lax.rem(digit + r - j, r)
                arriving[s].append((c, source))

    def run():
        for i in reversed(range(len(levels))):
            for c, digits in arriving[levels[i]]:
                c.wait_recv()
                forward(digits, levels[:i])

    forward(dict(enumerate(ctx["digits"])), levels)
    return run


def learn(basis, devices, parts, iters, deep, halves, chosen_ref, x_ref, res_ref, multi_ref, out_ref, active_ref, *scratch):
    scratch = list(scratch)
    resp, height = res_ref.shape[0], basis.height
    high = height // parts
    cands = multi_ref.shape[1]
    stages = radices(devices)
    me = lax.axis_index("samp")
    digits = [lax.rem(me // stride, r) for r, stride in stages]
    send, recv, twice, turned, rows, acc, total, gram, whole_gram, maps, hot = scratch[:11]
    buffers = scratch[11:]
    k = len(stages)
    take = lambda n: [buffers.pop(0) for _ in range(n)]
    part = take(parts)
    held = [take(k) for _ in range(parts)]
    landed = [take(k) for _ in range(parts)]
    gheld, glanded = take(k), take(k)

    barrier = pltpu.get_barrier_semaphore()
    peers = 0
    for (r, stride), digit in zip(stages, digits):
        for j in range(1, r):
            peer = me + (lax.rem(digit + j, r) - digit) * stride
            pl.semaphore_signal(barrier, inc=1, device_id=(peer,), device_id_type=MESH)
            peers += 1

    ctx = {"me": me, "digits": digits, "stages": stages, "sems": Semaphores(send, recv)}
    kept = up(iters, 4)
    unit = height // halves
    grams = Stream(ctx, gram, kept * halves, unit, gheld, glanded)
    streams = [Stream(ctx, part[p], resp, high, held[p], landed[p]) for p in range(parts)]

    prepare(basis, iters, chosen_ref, x_ref, res_ref, multi_ref, active_ref, twice, turned, rows)
    per = high * LANES // basis.stride
    for p in range(parts):
        blocks = basis.blocks[p * per : (p + 1) * per]
        correlate(basis, blocks, deep, twice, turned, rows, acc)
        count = len(blocks) * basis.stride // LANES
        for b in range(count):
            t = acc[b * LANES : (b + 1) * LANES, :].T
            corr = t[0:resp] + t[resp : 2 * resp]
            for q in range(0, resp, 8):
                part[p][pl.ds(q * high + b, 8, stride=high), :] = corr[q : q + 8]
            gram[pl.ds(p * high + b, 8, stride=height), :] = t[2 * resp : 2 * resp + 8]
        if count < high:
            res = res_ref[...]
            sq = jnp.broadcast_to(jnp.sum(res * res, axis=1, keepdims=True), (resp, LANES))
            for b in range(count, high):
                for q in range(0, resp, 8):
                    part[p][pl.ds(q * high + b, 8, stride=high), :] = sq[q : q + 8]
                gram[pl.ds(p * high + b, 8, stride=height), :] = jnp.zeros((8, LANES), jnp.float32)
        if p == 0:
            pl.semaphore_wait(barrier, peers)
        else:
            streams[p - 1].receive(0)
            if k > 1:
                streams[p - 1].send(1)
        streams[p].send(0)
    grams.send(0)

    line, lane = place(multi_ref[...], basis)
    maps[...] = jnp.zeros_like(maps)
    maps[0:1, 0:cands] = line
    maps[1:2, 0:cands] = lane
    for s in streams[parts - 1 :] + [grams]:
        s.receive(0)
        if k > 1:
            s.send(1)
    for c in range(0, maps.shape[1], LANES):
        at = maps[0:1, c : c + LANES]
        row = lax.broadcasted_iota(jnp.int32, (height, LANES), 0).astype(jnp.float32)
        one = jnp.where(row == at, 1.0, 0.0).astype(jnp.bfloat16)
        for i in range(3):
            hot[i * height : (i + 1) * height, c : c + LANES] = one
    for stage in range(1, k):
        for s in streams + [grams]:
            s.receive(stage)
            if stage + 1 < k:
                s.send(stage + 1)

    gplan, plan = grams.plan, streams[0].plan
    at = pl.multiple_of(digit_place(ctx, gplan, digits) * unit, 8)
    whole_gram[pl.ds(at, gplan[-1][1] * unit), :] = grams.now[...]
    run_gram = spread(ctx, gplan, unit, whole_gram)

    def arrange(row, store):
        first, rest = split(row)
        _, third = split(row - first.astype(jnp.float32))
        stacked = jnp.concatenate([first, rest, third], axis=0)
        wide = 4 * LANES
        for c in range(0, maps.shape[1], wide):
            size = min(wide, maps.shape[1] - c)
            found = lax.dot_general(
                stacked, hot[:, c : c + size], TN, preferred_element_type=jnp.float32
            )
            for i in range(0, size, LANES):
                at = maps[1:2, c + i : c + i + LANES]
                lo = lax.broadcasted_iota(jnp.int32, (LANES, LANES), 0).astype(jnp.float32)
                kept = jnp.where(lo == at, found[:, i : i + LANES], 0.0)
                store((c + i) // LANES, jnp.sum(kept, axis=0, keepdims=True))

    mine = digit_place(ctx, plan, digits) * height
    for i in range(plan[-1][1]):
        row = jnp.concatenate([s.now[i * high : (i + 1) * high, :] for s in streams], axis=0)
        lines = [row[height - 1 :]] * (height - maps.shape[1] // LANES)
        found = {}
        arrange(row, found.__setitem__)
        row = jnp.concatenate([found[b] for b in range(len(found))] + lines, axis=0)
        total[pl.ds(pl.multiple_of(mine + i * height, 8), height), :] = row
    run = spread(ctx, plan, height, total)
    run_gram()
    for g in range(iters):
        row = whole_gram[g * height : (g + 1) * height, :]
        found = {}
        arrange(row, found.__setitem__)
        lines = [row[height - 1 :]] * (height - len(found))
        out_ref[(resp + g) * height : (resp + g + 1) * height, :] = jnp.concatenate(
            [found[b] for b in range(len(found))] + lines, axis=0
        )
    run()
    rest = out_ref.shape[0] - (resp + iters) * height
    out_ref[(resp + iters) * height :, :] = jnp.zeros((rest, LANES), jnp.float32)
    out_ref[0 : resp * height, :] = total[...]
    for c in ctx["sems"].sent:
        c.wait_send()


def finish(cands, samples, iters, height, chosen_ref, total_ref, res_ref, active_ref, out_ref, corr_ref, coef_ref, flat):
    resp = res_ref.shape[0]
    for b in range(flat.shape[1] // LANES):
        for q in range(0, flat.shape[0], 8):
            flat[q : q + 8, b * LANES : (b + 1) * LANES] = total_ref[
                pl.ds(q * height + b, 8, stride=height), :
            ]
    sq = jnp.concatenate(
        [total_ref[pl.ds(q * height + height - 1, 8, stride=height), :] for q in range(0, resp, 8)],
        axis=0,
    )[:, 0:1]
    total = flat[:, 0:cands]
    column = lax.broadcasted_iota(jnp.int32, total.shape, 1)
    picked = [
        jnp.sum(jnp.where(column == chosen_ref[i], total, 0.0), axis=1, keepdims=True)
        for i in range(iters)
    ]
    target = [p[0:resp] for p in picked]
    gram = [[picked[j][resp + i : resp + i + 1] for j in range(iters)] for i in range(iters)]
    tri = [[None] * iters for _ in range(iters)]
    for i in range(iters):
        for j in range(i + 1):
            s = gram[i][j]
            for m in range(j):
                s = s - tri[i][m] * tri[j][m]
            tri[i][j] = jnp.sqrt(s) if i == j else s / tri[j][j]
    corr = total[0:resp]
    rows = [total[resp + i : resp + i + 1] for i in range(iters)]
    coef = [jnp.zeros((resp, 1), jnp.float32) for _ in range(iters)]
    for k in range(iters):
        norm = math.sqrt(samples) * jnp.sqrt(sq / samples + 1e-06)
        corr_ref[k] = corr * (1.0 / norm)
        largest = jnp.max(jnp.abs(corr), axis=1, keepdims=True)
        gamma = jnp.abs(target[k]) / (largest + 1e-06)
        w = []
        for i in range(k + 1):
            s = target[i]
            for m in range(i):
                s = s - tri[i][m] * w[m]
            w.append(s / tri[i][i])
        for i in reversed(range(k + 1)):
            s = w[i]
            for m in range(i + 1, k + 1):
                s = s - tri[m][i] * w[m]
            w[i] = s / tri[i][i]
        step = [gamma * wi for wi in w]
        for i in range(k + 1):
            coef[i] = coef[i] + step[i]
        if k < iters - 1:
            gain = sum(wi * t for wi, t in zip(w, target))
            sq = jnp.maximum(sq - gamma * (2.0 - gamma) * gain, 0.0)
            target = [
                target[j] - sum(step[i] * gram[i][j] for i in range(k + 1)) for j in range(iters)
            ]
            for i in range(k + 1):
                corr = corr - step[i] * rows[i]
    res = res_ref[...]
    active = active_ref[...].astype(jnp.float32)
    for i in range(iters):
        res = res - coef[i] * active[i : i + 1]
    out_ref[...] = res
    shape = (resp, resp)
    eye = lax.broadcasted_iota(jnp.int32, shape, 0) == lax.broadcasted_iota(jnp.int32, shape, 1)
    lines = [jnp.sum(jnp.where(eye, c, 0.0), axis=0, keepdims=True) for c in coef]
    line = lax.broadcasted_iota(jnp.int32, coef_ref.shape, 0)
    coef_ref[...] = sum(jnp.where(line == i, lines[i], 0.0) for i in range(iters))


def on_device(inputs, response, multi_index, chosen):
    nvars, width = inputs.shape
    devices = lax.axis_size("samp")
    samples = width * devices
    cands = multi_index.shape[0]
    iters = chosen.shape[0]
    resp = response.shape[0]
    basis = Basis(nvars)
    height, stride = basis.height, basis.stride
    few = up(iters, 16)
    kept = up(iters, 4)
    extra = up(kept, 8)
    used = resp + extra
    multi = multi_index.T
    vmem = pl.BlockSpec(memory_space=pltpu.VMEM)
    smem = pl.BlockSpec(memory_space=pltpu.SMEM)
    deep = math.gcd(width, 512)
    halves, parts = 2, 3
    high, unit = height // parts, height // halves
    stages = radices(devices)
    plan, gplan = halving(resp, stages), halving(kept * halves, stages)
    copies = (parts + 1) * sum(r - 1 for r, _ in stages)
    copies += resp // plan[-1][1] + kept * halves // gplan[-1][1] - 2
    grid = up(cands, LANES)
    lines = lambda n: pltpu.VMEM((n, LANES), jnp.float32)
    held = [lines(c * high) for _, c in plan]
    landed = [lines(r * c * high) for (r, _), (_, c) in zip(stages, plan)]
    gheld = [lines(c * unit) for _, c in gplan]
    glanded = [lines(r * c * unit) for (r, _), (_, c) in zip(stages, gplan)]
    total, active = pl.pallas_call(
        functools.partial(learn, basis, devices, parts, iters, deep, halves),
        in_specs=[smem, vmem, vmem, vmem],
        out_specs=[vmem, vmem],
        out_shape=[
            jax.ShapeDtypeStruct((used * height, LANES), jnp.float32),
            jax.ShapeDtypeStruct((few, width), jnp.bfloat16),
        ],
        scratch_shapes=[
            pltpu.SemaphoreType.DMA((copies,)),
            pltpu.SemaphoreType.DMA((copies,)),
            pltpu.VMEM((3 * stride, width), jnp.float32),
            pltpu.VMEM((2 * nvars * stride, width), jnp.float32),
            pltpu.VMEM((up(2 * resp + few, LANES), width), jnp.bfloat16),
            lines(high * LANES),
            lines(resp * height),
            lines(up(kept, 8) * height),
            lines(kept * height),
            pltpu.VMEM((8, grid), jnp.float32),
            pltpu.VMEM((3 * height, grid), jnp.bfloat16),
            *[lines(resp * high) for _ in range(parts)],
            *(held * parts),
            *(landed * parts),
            *gheld,
            *glanded,
        ],
        compiler_params=pltpu.CompilerParams(
            vmem_limit_bytes=VMEM_LIMIT, collective_id=0, has_side_effects=True
        ),
        name="learn",
    )(chosen, inputs, response, multi)
    residual, corr, coef = pl.pallas_call(
        functools.partial(finish, cands, samples, iters, height),
        in_specs=[smem, vmem, vmem, vmem],
        out_specs=[vmem, vmem, vmem],
        out_shape=[
            jax.ShapeDtypeStruct((resp, width), jnp.float32),
            jax.ShapeDtypeStruct((iters, resp, cands), jnp.float32),
            jax.ShapeDtypeStruct((iters, resp), jnp.float32),
        ],
        scratch_shapes=[pltpu.VMEM((used, grid), jnp.float32)],
        compiler_params=pltpu.CompilerParams(vmem_limit_bytes=VMEM_LIMIT),
        name="finish",
    )(chosen, total, response, active)
    return residual, corr, coef


def solution(mesh):
    placed = (P(None, "samp"), P(None, "samp"), P(), P())
    return jax.shard_map(
        on_device,
        mesh=mesh,
        in_specs=placed,
        out_specs=(P(None, "samp"), P(), P()),
        check_vma=False,
    )
```

```python
import functools
import math

import jax
import jax.numpy as jnp
from jax import lax
from jax.experimental import pallas as pl
from jax.experimental.pallas import tpu as pltpu
from jax.sharding import PartitionSpec as P

LANES = 128
NT = (((1,), (1,)), ((), ()))
TN = (((0,), (0,)), ((), ()))
MESH = pl.DeviceIdType.MESH
VMEM_LIMIT = 57 * 2**20


def up(n, m):
    return -(-n // m) * m


def split(x):
    high = x.astype(jnp.bfloat16)
    return high, (x - high.astype(jnp.float32)).astype(jnp.bfloat16)


class Basis:
    def __init__(self, nvars):
        self.nvars = nvars
        self.stride = up(nvars + 1, 16)
        gaps = []
        d = 1
        while nvars - 3 * d > 0:
            gaps += [(d, e) for e in range(d, nvars - 2 * d)]
            d += 1
        if nvars % 3 == 0:
            gaps.append((nvars // 3, nvars // 3))
        self.triples = len(gaps)
        self.pairs = nvars // 2
        self.squares = nvars - 1
        self.blocks = [("triple", d, d + e) for d, e in gaps]
        self.blocks += [("pair", d, 0) for d in range(1, self.pairs + 1)]
        self.blocks += [("square", d, 0) for d in range(1, self.squares + 1)]
        self.blocks += [("single", e, 0) for e in range(3)]
        while len(self.blocks) * self.stride % LANES:
            self.blocks.append(("single", 0, 0))
        self.lines = len(self.blocks) * self.stride // LANES
        self.height = up(self.lines + 1, 48)


def place(multi, basis):
    n = float(basis.nvars)
    deg = multi.astype(jnp.float32)
    var = lax.broadcasted_iota(jnp.int32, multi.shape, 0).astype(jnp.float32)
    pos = deg > 0.0
    down = lambda f, x: f(x, axis=0, keepdims=True)
    count = down(jnp.sum, jnp.where(pos, 1.0, 0.0))
    total = down(jnp.sum, jnp.where(pos, var, 0.0))
    low = down(jnp.min, jnp.where(pos, var, n))
    high = down(jnp.max, jnp.where(pos, var, 0.0))
    most = down(jnp.max, deg)
    two = down(jnp.sum, jnp.where(deg > 1.5, var, 0.0))
    mid = total - low - high
    g1, g2 = mid - low, high - mid
    g3 = n - g1 - g2
    at_mid = jnp.logical_and(g2 <= g3, g2 < g1)
    at_high = jnp.logical_and(g3 <= g1, g3 < g2)
    pick = lambda a, b, c: jnp.where(at_high, c, jnp.where(at_mid, b, a))
    d1, d2, start3 = pick(g1, g2, g3), pick(g2, g3, g1), pick(low, mid, high)
    block3 = n * (d1 - 1.0) - 1.5 * d1 * (d1 - 1.0) + d2 - d1
    gap = high - low
    near = gap <= n - gap
    block2 = float(basis.triples - 1) + jnp.where(near, gap, n - gap)
    start2 = jnp.where(near, low, high)
    one = total - two
    turn = two - one
    block21 = float(basis.triples + basis.pairs - 1) + jnp.where(turn > 0.0, turn, turn + n)
    base = float(basis.triples + basis.pairs + basis.squares)
    block1 = base + jnp.maximum(most - 1.0, 0.0)
    squared = most > 1.5
    block = jnp.where(
        count > 2.5, block3, jnp.where(count > 1.5, jnp.where(squared, block21, block2), block1)
    )
    start = jnp.where(
        count > 2.5, start3, jnp.where(count > 1.5, jnp.where(squared, one, start2), low)
    )
    index = block * float(basis.stride) + start
    line = jnp.floor(index * (1.0 / LANES))
    return line, index - line * float(LANES)


def prepare(basis, iters, loads, chosen_ref, x_ref, res_ref, multi_ref, active_ref, twice, turned, rows):
    nvars, width = x_ref.shape
    resp = res_ref.shape[0]
    stride = basis.stride
    few = active_ref.shape[0]
    loads[0].wait()
    x = x_ref[...]
    second = (3.0 * x * x - 1.0) * 0.5
    third = (5.0 * x * x * x - 3.0 * x) * 0.5
    values = [x * math.sqrt(3.0), second * math.sqrt(5.0), third * math.sqrt(7.0)]
    for e, value in enumerate(values):
        twice[e * stride + nvars : (e + 1) * stride, :] = jnp.ones((stride - nvars, width), jnp.float32)
        twice[e * stride : e * stride + nvars, :] = value
    zero = jnp.zeros((stride - nvars, width), jnp.float32)
    for e in range(2):
        for d in range(1, nvars):
            at = (e * nvars + d) * stride
            turned[at : at + nvars - d, :] = values[e][d:]
            turned[at + nvars - d : at + nvars, :] = values[e][:d]
            turned[at + nvars : at + stride, :] = zero

    loads[1].wait()
    loads[2].wait()
    high, low = split(res_ref[...])
    rows[0:resp, :] = high
    rows[resp : 2 * resp, :] = low
    multi = multi_ref[...]
    column = lax.broadcasted_iota(jnp.int32, multi.shape, 1)
    line = lax.broadcasted_iota(jnp.int32, (few, width), 0)
    actives = jnp.zeros((few, width), jnp.float32)
    for k in range(iters):
        deg = jnp.sum(
            jnp.where(column == chosen_ref[k], multi, 0).astype(jnp.float32), axis=1, keepdims=True
        )
        v = jnp.where(
            deg > 2.5,
            values[2],
            jnp.where(deg > 1.5, values[1], jnp.where(deg > 0.5, values[0], 1.0)),
        )
        p = v[0:8]
        for i in range(8, nvars - 7, 8):
            p = p * v[i : i + 8]
        row = p[0:1]
        for i in range(1, min(8, nvars)):
            row = row * p[i : i + 1]
        for i in range(nvars // 8 * 8, nvars):
            row = row * v[i : i + 1]
        actives = jnp.where(line == k, row, actives)
    actives = actives.astype(jnp.bfloat16)
    active_ref[...] = actives
    rows[2 * resp : 2 * resp + few, :] = actives
    rest = rows.shape[0] - 2 * resp - few
    rows[2 * resp + few :, :] = jnp.zeros((rest, width), jnp.bfloat16)


def correlate(basis, blocks, deep, twice, turned, rows, acc):
    stride, nvars = basis.stride, basis.nvars
    width = rows.shape[1]
    per = 512 // stride
    groups = [blocks[i : i + per] for i in range(0, len(blocks), per)]

    def step(k, first):
        for g, group in enumerate(groups):
            total = None
            for half in range(0, deep, 256):
                at = k * deep + half
                cols = pl.ds(at if first else pl.multiple_of(at, 256), 256)
                f1 = twice[0:stride, cols]
                parts = []
                held = None
                for kind, d, e in group:
                    if kind == "triple":
                        if held != d:
                            pair = f1 * turned[d * stride : (d + 1) * stride, cols]
                            held = d
                        part = pair * turned[e * stride : (e + 1) * stride, cols]
                    elif kind == "pair":
                        part = f1 * turned[d * stride : (d + 1) * stride, cols]
                    elif kind == "square":
                        part = f1 * turned[(nvars + d) * stride : (nvars + d + 1) * stride, cols]
                    else:
                        part = twice[d * stride : (d + 1) * stride, cols]
                    parts.append(part.astype(jnp.bfloat16))
                psi = jnp.concatenate(parts, axis=0)
                term = lax.dot_general(psi, rows[:, cols], NT, preferred_element_type=jnp.float32)
                total = term if total is None else total + term
            span = slice(g * per * stride, (g * per + len(group)) * stride)
            acc[span, :] = total if first else acc[span, :] + total

    step(0, True)

    if width > deep:

        @pl.loop(1, width // deep)
        def _(k):
            step(k, False)


def radices(n):
    result, stride = [], 1
    while n > 1:
        r = 2 if stride == 1 or n == 2 else 4
        if n % r:
            raise ValueError("device count")
        result.append((r, stride))
        stride *= r
        n //= r
    return result


def halving(count, stages):
    plan = []
    for r, _ in stages:
        cut = count % r == 0
        count = count // r if cut else count
        plan.append((cut, count))
    return plan


class Semaphores:
    def __init__(self, send, recv):
        self.send, self.recv, self.used, self.sent = send, recv, 0, []

    def copy(self, src, dst, peer):
        c = pltpu.make_async_remote_copy(
            src_ref=src,
            dst_ref=dst,
            send_sem=self.send.at[self.used],
            recv_sem=self.recv.at[self.used],
            device_id=(peer,),
            device_id_type=MESH,
        )
        self.used += 1
        self.sent.append(c)
        c.start()
        return c


class Stream:
    def __init__(self, ctx, part, count, unit, held, landed):
        self.ctx, self.unit = ctx, unit
        self.now = part
        self.held, self.landed = held, landed
        self.plan = halving(count, ctx["stages"])
        self.waiting = None

    def send(self, s):
        r, stride = self.ctx["stages"][s]
        digit = self.ctx["digits"][s]
        cut, count = self.plan[s]
        size = count * self.unit
        copies = []
        for j in range(r - 1, 0, -1):
            other = lax.rem(digit + j, r)
            peer = self.ctx["me"] + (other - digit) * stride
            at = pl.multiple_of(other * size, 8) if cut else 0
            copies.append(
                self.ctx["sems"].copy(
                    self.now.at[pl.ds(at, size)], self.landed[s].at[pl.ds(j * size, size)], peer
                )
            )
        self.waiting = copies

    def receive(self, s):
        r, _ = self.ctx["stages"][s]
        digit = self.ctx["digits"][s]
        cut, count = self.plan[s]
        size = count * self.unit
        for c in self.waiting:
            c.wait_recv()
        at = pl.multiple_of(digit * size, 8) if cut else 0
        own = self.now[pl.ds(at, size), :]
        landed = self.landed[s]
        if cut:
            total = own
            for j in range(1, r):
                total = total + landed[j * size : (j + 1) * size, :]
        else:
            landed[0:size, :] = own
            total = None
            for i in range(r):
                at = pl.multiple_of(lax.rem(digit + r - i, r) * size, 8)
                term = landed[pl.ds(at, size), :]
                total = term if total is None else total + term
        self.held[s][...] = total
        self.now = self.held[s]


def digit_place(ctx, plan, digits):
    at, weight = 0, plan[-1][1]
    for s in reversed(range(len(plan))):
        if plan[s][0]:
            at = at + digits[s] * weight
            weight *= ctx["stages"][s][0]
    return at


def spread(ctx, plan, unit, tall, whole):
    levels = [s for s, (cut, _) in enumerate(plan) if cut]
    size = (plan[-1][1] - 1) * unit + tall
    arriving = {s: [] for s in levels}

    def forward(digits, below):
        at = pl.multiple_of(digit_place(ctx, plan, digits) * unit, 8)
        block = whole.at[pl.ds(at, size)]
        for s in reversed(below):
            r, stride = ctx["stages"][s]
            digit = ctx["digits"][s]
            for j in range(r - 1, 0, -1):
                peer = ctx["me"] + (lax.rem(digit + j, r) - digit) * stride
                c = ctx["sems"].copy(block, block, peer)
                source = dict(digits)
                source[s] = lax.rem(digit + r - j, r)
                arriving[s].append((c, source))

    forward(dict(enumerate(ctx["digits"])), levels)

    def run():
        for i in reversed(range(len(levels))):
            for c, digits in arriving[levels[i]]:
                c.wait_recv()
                forward(digits, levels[:i])
                yield levels[i]

    return run()


def learn(basis, devices, parts, iters, deep, halves, tile, chosen_ref, x_in, res_in, multi_in, out_ref, active_ref, *scratch):
    scratch = list(scratch)
    resp, height = res_in.shape[0], basis.height
    high = height // parts
    cands = multi_in.shape[1]
    stages = radices(devices)
    me = lax.axis_index("samp")
    digits = [lax.rem(me // stride, r) for r, stride in stages]
    send, recv, loaded, x_ref, res_ref, multi_ref, twice, turned, rows, acc, total, maps, hot = scratch[:13]
    buffers = scratch[13:]
    loads = []
    for i, (a, b) in enumerate([(x_in, x_ref), (multi_in, multi_ref), (res_in, res_ref)]):
        loads.append(pltpu.make_async_copy(a, b, loaded.at[i]))
        loads[-1].start()
    k = len(stages)
    take = lambda n: [buffers.pop(0) for _ in range(n)]
    part = take(parts)
    held = [take(k) for _ in range(parts)]
    landed = [take(k) for _ in range(parts)]
    pieces = parts // 2
    gram, whole_gram = take(pieces), take(pieces)
    gheld = [take(k) for _ in range(pieces)]
    glanded = [take(k) for _ in range(pieces)]

    barrier = pltpu.get_barrier_semaphore()
    peers = 0
    for (r, stride), digit in zip(stages, digits):
        for j in range(1, r):
            peer = me + (lax.rem(digit + j, r) - digit) * stride
            pl.semaphore_signal(barrier, inc=1, device_id=(peer,), device_id_type=MESH)
            peers += 1

    ctx = {"me": me, "digits": digits, "stages": stages, "sems": Semaphores(send, recv)}
    kept = up(iters, 4)
    unit = 2 * high // halves
    grams = [
        Stream(ctx, gram[g], kept * halves, unit, gheld[g], glanded[g]) for g in range(pieces)
    ]
    streams = [Stream(ctx, part[p], resp, high, held[p], landed[p]) for p in range(parts)]

    prepare(basis, iters, loads, chosen_ref, x_ref, res_ref, multi_ref, active_ref, twice, turned, rows)
    per = high * LANES // basis.stride
    hold = 1
    flying = []
    for p in range(parts):
        blocks = basis.blocks[p * per : (p + 1) * per]
        correlate(basis, blocks, deep, twice, turned, rows, acc)
        count = len(blocks) * basis.stride // LANES
        for b in range(count):
            t = acc[b * LANES : (b + 1) * LANES, :].T
            corr = t[0:resp] + t[resp : 2 * resp]
            for q in range(0, resp, 8):
                part[p][pl.ds(q * high + b, 8, stride=high), :] = corr[q : q + 8]
            gram[p // 2][pl.ds(p % 2 * high + b, 8, stride=2 * high), :] = t[2 * resp : 2 * resp + 8]
        if count < high:
            res = res_ref[...]
            sq = jnp.broadcast_to(jnp.sum(res * res, axis=1, keepdims=True), (resp, LANES))
            for b in range(count, high):
                for q in range(0, resp, 8):
                    part[p][pl.ds(q * high + b, 8, stride=high), :] = sq[q : q + 8]
                gram[p // 2][pl.ds(p % 2 * high + b, 8, stride=2 * high), :] = jnp.zeros(
                    (8, LANES), jnp.float32
                )
        if p < hold:
            continue
        if p == hold:
            pl.semaphore_wait(barrier, peers)
        sent, flying = flying, []
        for s in sent:
            s.receive(0)
            if k > 1:
                s.send(1)
        for i in range(p + 1) if p == hold else [p]:
            flying.append(streams[i])
            if i % 2:
                flying.append(grams[i // 2])
        for s in flying:
            s.send(0)

    line, lane = place(multi_ref[...], basis)
    maps[...] = jnp.zeros_like(maps)
    maps[0:1, 0:cands] = line
    maps[1:2, 0:cands] = lane
    for s in flying:
        s.receive(0)
        if k > 1:
            s.send(1)
    for c in range(0, maps.shape[1], LANES):
        at = maps[0:1, c : c + LANES]
        row = lax.broadcasted_iota(jnp.int32, (height, LANES), 0).astype(jnp.float32)
        one = jnp.where(row == at, 1.0, 0.0).astype(jnp.bfloat16)
        for i in range(3):
            hot[i * height : (i + 1) * height, c : c + LANES] = one
    order = []
    for p in range(parts):
        order.append(streams[p])
        if p % 2:
            order.append(grams[p // 2])
    for stage in range(1, k):
        for s in order:
            s.receive(stage)
            if stage + 1 < k:
                s.send(stage + 1)

    gplan, plan = grams[0].plan, streams[0].plan
    at = pl.multiple_of(digit_place(ctx, gplan, digits) * unit, 8)
    runs = []
    for g in range(pieces):
        whole_gram[g][pl.ds(at, gplan[-1][1] * unit), :] = grams[g].now[...]
        runs.append(spread(ctx, gplan, unit, unit, whole_gram[g]))

    def arrange(row, store):
        first, rest = split(row)
        _, third = split(row - first.astype(jnp.float32))
        stacked = jnp.concatenate([first, rest, third], axis=0)
        wide = 4 * LANES
        for c in range(0, maps.shape[1], wide):
            size = min(wide, maps.shape[1] - c)
            found = lax.dot_general(
                stacked, hot[:, c : c + size], TN, preferred_element_type=jnp.float32
            )
            for i in range(0, size, LANES):
                at = maps[1:2, c + i : c + i + LANES]
                lo = lax.broadcasted_iota(jnp.int32, (LANES, LANES), 0).astype(jnp.float32)
                kept = jnp.where(lo == at, found[:, i : i + LANES], 0.0)
                store((c + i) // LANES, jnp.sum(kept, axis=0, keepdims=True))

    mine = digit_place(ctx, plan, digits) * height

    def arranged(row):
        found = {}
        arrange(row, found.__setitem__)
        lines = [row[height - 1 :]] * (height - len(found))
        return jnp.concatenate([found[b] for b in range(len(found))] + lines, axis=0)

    for i in range(plan[-1][1]):
        row = jnp.concatenate([s.now[i * high : (i + 1) * high, :] for s in streams], axis=0)
        total[pl.ds(pl.multiple_of(mine + i * height, 8), height), :] = arranged(row)
    run = spread(ctx, plan, height, up(maps.shape[1] // LANES + 1, tile), total)
    last = [s for s, (cut, _) in enumerate(plan) if cut][-1]
    todo = list(range(iters))

    def gram_row():
        if len(todo) == iters:
            for r in runs:
                for _ in r:
                    pass
        g = todo.pop(0)
        span = slice(g * 2 * high, (g + 1) * 2 * high)
        row = jnp.concatenate([w[span, :] for w in whole_gram], axis=0)
        out_ref[(resp + g) * height : (resp + g + 1) * height, :] = arranged(row)

    since = 0
    for level in run:
        if level == last:
            continue
        since += 1
        if todo and since % 3 == 0:
            gram_row()
    while todo:
        gram_row()
    rest = out_ref.shape[0] - (resp + iters) * height
    out_ref[(resp + iters) * height :, :] = jnp.zeros((rest, LANES), jnp.float32)
    out_ref[0 : resp * height, :] = total[...]
    for c in ctx["sems"].sent:
        c.wait_send()


def finish(cands, samples, iters, height, chosen_ref, total_ref, res_ref, active_ref, out_ref, corr_out, coef_ref, flat, corr_ref, sems):
    resp = res_ref.shape[0]
    for b in range(flat.shape[1] // LANES):
        for q in range(0, flat.shape[0], 8):
            flat[q : q + 8, b * LANES : (b + 1) * LANES] = total_ref[
                pl.ds(q * height + b, 8, stride=height), :
            ]
    sq = jnp.concatenate(
        [
            total_ref[pl.ds(q * height + flat.shape[1] // LANES, 8, stride=height), :]
            for q in range(0, resp, 8)
        ],
        axis=0,
    )[:, 0:1]
    total = flat[:, 0:cands]
    column = lax.broadcasted_iota(jnp.int32, total.shape, 1)
    picked = [
        jnp.sum(jnp.where(column == chosen_ref[i], total, 0.0), axis=1, keepdims=True)
        for i in range(iters)
    ]
    target = [p[0:resp] for p in picked]
    gram = [[picked[j][resp + i : resp + i + 1] for j in range(iters)] for i in range(iters)]
    tri = [[None] * iters for _ in range(iters)]
    for i in range(iters):
        for j in range(i + 1):
            s = gram[i][j]
            for m in range(j):
                s = s - tri[i][m] * tri[j][m]
            tri[i][j] = jnp.sqrt(s) if i == j else s / tri[j][j]
    corr = total[0:resp]
    rows = [total[resp + i : resp + i + 1] for i in range(iters)]
    coef = [jnp.zeros((resp, 1), jnp.float32) for _ in range(iters)]
    copies = []
    for k in range(iters):
        norm = math.sqrt(samples) * jnp.sqrt(sq / samples + 1e-06)
        corr_ref[k] = corr * (1.0 / norm)
        copies.append(pltpu.make_async_copy(corr_ref.at[k], corr_out.at[k], sems.at[k]))
        copies[-1].start()
        largest = jnp.max(jnp.abs(corr), axis=1, keepdims=True)
        gamma = jnp.abs(target[k]) / (largest + 1e-06)
        w = []
        for i in range(k + 1):
            s = target[i]
            for m in range(i):
                s = s - tri[i][m] * w[m]
            w.append(s / tri[i][i])
        for i in reversed(range(k + 1)):
            s = w[i]
            for m in range(i + 1, k + 1):
                s = s - tri[m][i] * w[m]
            w[i] = s / tri[i][i]
        step = [gamma * wi for wi in w]
        for i in range(k + 1):
            coef[i] = coef[i] + step[i]
        if k < iters - 1:
            gain = sum(wi * t for wi, t in zip(w, target))
            sq = jnp.maximum(sq - gamma * (2.0 - gamma) * gain, 0.0)
            target = [
                target[j] - sum(step[i] * gram[i][j] for i in range(k + 1)) for j in range(iters)
            ]
            for i in range(k + 1):
                corr = corr - step[i] * rows[i]
    res = res_ref[...]
    active = active_ref[...].astype(jnp.float32)
    for i in range(iters):
        res = res - coef[i] * active[i : i + 1]
    out_ref[...] = res
    shape = (resp, resp)
    eye = lax.broadcasted_iota(jnp.int32, shape, 0) == lax.broadcasted_iota(jnp.int32, shape, 1)
    lines = [jnp.sum(jnp.where(eye, c, 0.0), axis=0, keepdims=True) for c in coef]
    line = lax.broadcasted_iota(jnp.int32, coef_ref.shape, 0)
    coef_ref[...] = sum(jnp.where(line == i, lines[i], 0.0) for i in range(iters))
    for c in copies:
        c.wait()


def on_device(inputs, response, multi_index, chosen):
    nvars, width = inputs.shape
    devices = lax.axis_size("samp")
    samples = width * devices
    cands = multi_index.shape[0]
    iters = chosen.shape[0]
    resp = response.shape[0]
    basis = Basis(nvars)
    height, stride = basis.height, basis.stride
    few = up(iters, 16)
    kept = up(iters, 4)
    extra = up(kept, 8)
    used = resp + extra
    multi = multi_index.T
    vmem = pl.BlockSpec(memory_space=pltpu.VMEM)
    smem = pl.BlockSpec(memory_space=pltpu.SMEM)
    hbm = pl.BlockSpec(memory_space=pltpu.HBM)
    deep = width
    halves, parts, tile = 2, 6, 4
    high = height // parts
    unit, pieces = 2 * high // halves, parts // 2
    stages = radices(devices)
    plan, gplan = halving(resp, stages), halving(kept * halves, stages)
    copies = (parts + pieces) * sum(r - 1 for r, _ in stages)
    copies += resp // plan[-1][1] - 1 + pieces * (kept * halves // gplan[-1][1] - 1)
    grid = up(cands, LANES)
    lines = lambda n: pltpu.VMEM((n, LANES), jnp.float32)
    held = [lines(c * high) for _, c in plan]
    landed = [lines(r * c * high) for (r, _), (_, c) in zip(stages, plan)]
    gheld = [lines(c * unit) for _, c in gplan]
    glanded = [lines(r * c * unit) for (r, _), (_, c) in zip(stages, gplan)]
    total, active = pl.pallas_call(
        functools.partial(learn, basis, devices, parts, iters, deep, halves, tile),
        in_specs=[smem, hbm, hbm, hbm],
        out_specs=[vmem, vmem],
        out_shape=[
            jax.ShapeDtypeStruct((used * height, LANES), jnp.float32),
            jax.ShapeDtypeStruct((few, width), jnp.bfloat16),
        ],
        scratch_shapes=[
            pltpu.SemaphoreType.DMA((copies,)),
            pltpu.SemaphoreType.DMA((copies,)),
            pltpu.SemaphoreType.DMA((3,)),
            pltpu.VMEM(inputs.shape, jnp.float32),
            pltpu.VMEM(response.shape, jnp.float32),
            pltpu.VMEM(multi.shape, jnp.int32),
            pltpu.VMEM((3 * stride, width), jnp.float32),
            pltpu.VMEM((2 * nvars * stride, width), jnp.float32),
            pltpu.VMEM((up(2 * resp + few, LANES), width), jnp.bfloat16),
            lines(high * LANES),
            lines(resp * height),
            pltpu.VMEM((8, grid), jnp.float32),
            pltpu.VMEM((3 * height, grid), jnp.bfloat16),
            *[lines(resp * high) for _ in range(parts)],
            *(held * parts),
            *(landed * parts),
            *[lines(up(kept, 8) * 2 * high) for _ in range(pieces)],
            *[lines(kept * 2 * high) for _ in range(pieces)],
            *(gheld * pieces),
            *(glanded * pieces),
        ],
        compiler_params=pltpu.CompilerParams(
            vmem_limit_bytes=VMEM_LIMIT, collective_id=0, has_side_effects=True
        ),
        name="learn",
    )(chosen, inputs, response, multi)
    residual, corr, coef = pl.pallas_call(
        functools.partial(finish, cands, samples, iters, height),
        in_specs=[smem, vmem, vmem, vmem],
        out_specs=[vmem, pl.BlockSpec(memory_space=pl.ANY), vmem],
        out_shape=[
            jax.ShapeDtypeStruct((resp, width), jnp.float32),
            jax.ShapeDtypeStruct((iters, resp, cands), jnp.float32),
            jax.ShapeDtypeStruct((iters, resp), jnp.float32),
        ],
        scratch_shapes=[
            pltpu.VMEM((used, grid), jnp.float32),
            pltpu.VMEM((iters, resp, cands), jnp.float32),
            pltpu.SemaphoreType.DMA((iters,)),
        ],
        compiler_params=pltpu.CompilerParams(vmem_limit_bytes=VMEM_LIMIT),
        name="finish",
    )(chosen, total, response, active)
    return residual, corr, coef


def solution(mesh):
    placed = (P(None, "samp"), P(None, "samp"), P(), P())
    return jax.shard_map(
        on_device,
        mesh=mesh,
        in_specs=placed,
        out_specs=(P(None, "samp"), P(), P()),
        check_vma=False,
    )
```

```python
import functools
import math

import jax
import jax.numpy as jnp
from jax import lax
from jax.experimental import pallas as pl
from jax.experimental.pallas import tpu as pltpu
from jax.sharding import PartitionSpec as P

LANES = 128
NT = (((1,), (1,)), ((), ()))
TN = (((0,), (0,)), ((), ()))
MESH = pl.DeviceIdType.MESH
VMEM_LIMIT = 57 * 2**20


def up(n, m):
    return -(-n // m) * m


def split(x):
    high = x.astype(jnp.bfloat16)
    return high, (x - high.astype(jnp.float32)).astype(jnp.bfloat16)


class Basis:
    def __init__(self, nvars):
        self.nvars = nvars
        self.stride = up(nvars + 1, 16)
        gaps = []
        d = 1
        while nvars - 3 * d > 0:
            gaps += [(d, e) for e in range(d, nvars - 2 * d)]
            d += 1
        if nvars % 3 == 0:
            gaps.append((nvars // 3, nvars // 3))
        self.triples = len(gaps)
        self.pairs = nvars // 2
        self.squares = nvars - 1
        self.blocks = [("triple", d, d + e) for d, e in gaps]
        self.blocks += [("pair", d, 0) for d in range(1, self.pairs + 1)]
        self.blocks += [("square", d, 0) for d in range(1, self.squares + 1)]
        self.blocks += [("single", e, 0) for e in range(3)]
        while len(self.blocks) * self.stride % LANES:
            self.blocks.append(("single", 0, 0))
        self.lines = len(self.blocks) * self.stride // LANES
        self.height = up(self.lines + 1, 48)


def place(multi, basis):
    n = float(basis.nvars)
    deg = multi.astype(jnp.float32)
    var = lax.broadcasted_iota(jnp.int32, multi.shape, 0).astype(jnp.float32)
    pos = deg > 0.0
    down = lambda f, x: f(x, axis=0, keepdims=True)
    count = down(jnp.sum, jnp.where(pos, 1.0, 0.0))
    total = down(jnp.sum, jnp.where(pos, var, 0.0))
    low = down(jnp.min, jnp.where(pos, var, n))
    high = down(jnp.max, jnp.where(pos, var, 0.0))
    most = down(jnp.max, deg)
    two = down(jnp.sum, jnp.where(deg > 1.5, var, 0.0))
    mid = total - low - high
    g1, g2 = mid - low, high - mid
    g3 = n - g1 - g2
    at_mid = jnp.logical_and(g2 <= g3, g2 < g1)
    at_high = jnp.logical_and(g3 <= g1, g3 < g2)
    pick = lambda a, b, c: jnp.where(at_high, c, jnp.where(at_mid, b, a))
    d1, d2, start3 = pick(g1, g2, g3), pick(g2, g3, g1), pick(low, mid, high)
    block3 = n * (d1 - 1.0) - 1.5 * d1 * (d1 - 1.0) + d2 - d1
    gap = high - low
    near = gap <= n - gap
    block2 = float(basis.triples - 1) + jnp.where(near, gap, n - gap)
    start2 = jnp.where(near, low, high)
    one = total - two
    turn = two - one
    block21 = float(basis.triples + basis.pairs - 1) + jnp.where(turn > 0.0, turn, turn + n)
    base = float(basis.triples + basis.pairs + basis.squares)
    block1 = base + jnp.maximum(most - 1.0, 0.0)
    squared = most > 1.5
    block = jnp.where(
        count > 2.5, block3, jnp.where(count > 1.5, jnp.where(squared, block21, block2), block1)
    )
    start = jnp.where(
        count > 2.5, start3, jnp.where(count > 1.5, jnp.where(squared, one, start2), low)
    )
    index = block * float(basis.stride) + start
    line = jnp.floor(index * (1.0 / LANES))
    return line, index - line * float(LANES)


def prepare(basis, iters, loads, chosen_ref, x_ref, res_ref, multi_ref, active_ref, twice, turned, rows):
    nvars, width = x_ref.shape
    resp = res_ref.shape[0]
    stride = basis.stride
    few = active_ref.shape[0]
    loads[0].wait()
    x = x_ref[...]
    second = (3.0 * x * x - 1.0) * 0.5
    third = (5.0 * x * x * x - 3.0 * x) * 0.5
    values = [x * math.sqrt(3.0), second * math.sqrt(5.0), third * math.sqrt(7.0)]
    for e, value in enumerate(values):
        twice[e * stride + nvars : (e + 1) * stride, :] = jnp.ones((stride - nvars, width), jnp.float32)
        twice[e * stride : e * stride + nvars, :] = value
    zero = jnp.zeros((stride - nvars, width), jnp.float32)
    for e in range(2):
        for d in range(1, nvars):
            at = (e * nvars + d) * stride
            turned[at : at + nvars - d, :] = values[e][d:]
            turned[at + nvars - d : at + nvars, :] = values[e][:d]
            turned[at + nvars : at + stride, :] = zero

    loads[1].wait()
    loads[2].wait()
    high, low = split(res_ref[...])
    rows[0:resp, :] = high
    rows[resp : 2 * resp, :] = low
    multi = multi_ref[...]
    column = lax.broadcasted_iota(jnp.int32, multi.shape, 1)
    line = lax.broadcasted_iota(jnp.int32, (few, width), 0)
    actives = jnp.zeros((few, width), jnp.float32)
    for k in range(iters):
        deg = jnp.sum(
            jnp.where(column == chosen_ref[k], multi, 0).astype(jnp.float32), axis=1, keepdims=True
        )
        v = jnp.where(
            deg > 2.5,
            values[2],
            jnp.where(deg > 1.5, values[1], jnp.where(deg > 0.5, values[0], 1.0)),
        )
        p = v[0:8]
        for i in range(8, nvars - 7, 8):
            p = p * v[i : i + 8]
        row = p[0:1]
        for i in range(1, min(8, nvars)):
            row = row * p[i : i + 1]
        for i in range(nvars // 8 * 8, nvars):
            row = row * v[i : i + 1]
        actives = jnp.where(line == k, row, actives)
    actives = actives.astype(jnp.bfloat16)
    active_ref[...] = actives
    rows[2 * resp : 2 * resp + few, :] = actives
    rest = rows.shape[0] - 2 * resp - few
    rows[2 * resp + few :, :] = jnp.zeros((rest, width), jnp.bfloat16)


def correlate(basis, blocks, deep, twice, turned, rows, acc):
    stride, nvars = basis.stride, basis.nvars
    width = rows.shape[1]
    per = 512 // stride
    groups = [blocks[i : i + per] for i in range(0, len(blocks), per)]

    def step(k, first):
        for g, group in enumerate(groups):
            total = None
            for half in range(0, deep, 256):
                at = k * deep + half
                cols = pl.ds(at if first else pl.multiple_of(at, 256), 256)
                f1 = twice[0:stride, cols]
                parts = []
                held = None
                for kind, d, e in group:
                    if kind == "triple":
                        if held != d:
                            pair = f1 * turned[d * stride : (d + 1) * stride, cols]
                            held = d
                        part = pair * turned[e * stride : (e + 1) * stride, cols]
                    elif kind == "pair":
                        part = f1 * turned[d * stride : (d + 1) * stride, cols]
                    elif kind == "square":
                        part = f1 * turned[(nvars + d) * stride : (nvars + d + 1) * stride, cols]
                    else:
                        part = twice[d * stride : (d + 1) * stride, cols]
                    parts.append(part.astype(jnp.bfloat16))
                psi = jnp.concatenate(parts, axis=0)
                term = lax.dot_general(psi, rows[:, cols], NT, preferred_element_type=jnp.float32)
                total = term if total is None else total + term
            span = slice(g * per * stride, (g * per + len(group)) * stride)
            acc[span, :] = total if first else acc[span, :] + total

    step(0, True)

    if width > deep:

        @pl.loop(1, width // deep)
        def _(k):
            step(k, False)


def radices(n):
    result, stride = [], 1
    while n > 1:
        r = 2 if stride == 1 or n == 2 else 4
        if n % r:
            raise ValueError("device count")
        result.append((r, stride))
        stride *= r
        n //= r
    return result


def partner(digit, j, r):
    result, bit = 0, 1
    while bit < r:
        b = lax.rem(digit // bit, 2)
        result = result + bit * (1 - b if j & bit else b)
        bit *= 2
    return result


def halving(count, stages):
    plan = []
    for r, _ in stages:
        cut = count % r == 0
        count = count // r if cut else count
        plan.append((cut, count))
    return plan


class Semaphores:
    def __init__(self, send, recv):
        self.send, self.recv, self.used, self.sent = send, recv, 0, []

    def copy(self, src, dst, peer):
        c = pltpu.make_async_remote_copy(
            src_ref=src,
            dst_ref=dst,
            send_sem=self.send.at[self.used],
            recv_sem=self.recv.at[self.used],
            device_id=(peer,),
            device_id_type=MESH,
        )
        self.used += 1
        self.sent.append(c)
        c.start()
        return c


class Stream:
    def __init__(self, ctx, part, count, unit, held, landed):
        self.ctx, self.unit = ctx, unit
        self.now = part
        self.held, self.landed = held, landed
        self.plan = halving(count, ctx["stages"])
        self.waiting = None

    def send(self, s):
        r, stride = self.ctx["stages"][s]
        digit = self.ctx["digits"][s]
        cut, count = self.plan[s]
        size = count * self.unit
        copies = []
        for j in range(r - 1, 0, -1):
            other = partner(digit, j, r)
            peer = self.ctx["me"] + (other - digit) * stride
            at = pl.multiple_of(other * size, 8) if cut else 0
            copies.append(
                self.ctx["sems"].copy(
                    self.now.at[pl.ds(at, size)], self.landed[s].at[pl.ds(j * size, size)], peer
                )
            )
        self.waiting = copies

    def receive(self, s):
        r, _ = self.ctx["stages"][s]
        digit = self.ctx["digits"][s]
        cut, count = self.plan[s]
        size = count * self.unit
        for c in self.waiting:
            c.wait_recv()
        at = pl.multiple_of(digit * size, 8) if cut else 0
        own = self.now[pl.ds(at, size), :]
        landed = self.landed[s]
        if cut:
            total = own
            for j in range(1, r):
                total = total + landed[j * size : (j + 1) * size, :]
        else:
            landed[0:size, :] = own
            total = None
            for i in range(r):
                at = pl.multiple_of(partner(digit, i, r) * size, 8)
                term = landed[pl.ds(at, size), :]
                total = term if total is None else total + term
        self.held[s][...] = total
        self.now = self.held[s]


def digit_place(ctx, plan, digits):
    at, weight = 0, plan[-1][1]
    for s in reversed(range(len(plan))):
        if plan[s][0]:
            at = at + digits[s] * weight
            weight *= ctx["stages"][s][0]
    return at


def spread(ctx, plan, unit, tall, whole):
    levels = [s for s, (cut, _) in enumerate(plan) if cut]
    size = (plan[-1][1] - 1) * unit + tall
    arriving = {s: [] for s in levels}

    def forward(digits, below):
        at = pl.multiple_of(digit_place(ctx, plan, digits) * unit, 8)
        block = whole.at[pl.ds(at, size)]
        for s in reversed(below):
            r, stride = ctx["stages"][s]
            digit = ctx["digits"][s]
            arrivals = []
            for j in range(r - 1, 0, -1):
                peer = ctx["me"] + (partner(digit, j, r) - digit) * stride
                c = ctx["sems"].copy(block, block, peer)
                source = dict(digits)
                source[s] = partner(digit, j, r)
                arrivals.insert(0, (c, source))
            arriving[s] += arrivals

    forward(dict(enumerate(ctx["digits"])), levels)

    def run():
        for i in reversed(range(len(levels))):
            for c, digits in arriving[levels[i]]:
                c.wait_recv()
                forward(digits, levels[:i])
                yield levels[i]

    return run()


def learn(basis, devices, parts, iters, deep, halves, tile, chosen_ref, x_in, res_in, multi_in, out_ref, active_ref, *scratch):
    scratch = list(scratch)
    resp, height = res_in.shape[0], basis.height
    high = height // parts
    cands = multi_in.shape[1]
    stages = radices(devices)
    me = lax.axis_index("samp")
    digits = [lax.rem(me // stride, r) for r, stride in stages]
    send, recv, loaded, x_ref, res_ref, multi_ref, twice, turned, rows, acc, total, maps, hot = scratch[:13]
    buffers = scratch[13:]
    loads = []
    for i, (a, b) in enumerate([(x_in, x_ref), (multi_in, multi_ref), (res_in, res_ref)]):
        loads.append(pltpu.make_async_copy(a, b, loaded.at[i]))
        loads[-1].start()
    k = len(stages)
    take = lambda n: [buffers.pop(0) for _ in range(n)]
    part = take(parts)
    held = [take(k) for _ in range(parts)]
    landed = [take(k) for _ in range(parts)]
    pieces = parts // 2
    gram, whole_gram = take(pieces), take(pieces)
    gheld = [take(k) for _ in range(pieces)]
    glanded = [take(k) for _ in range(pieces)]

    barrier = pltpu.get_barrier_semaphore()
    peers = 0
    for (r, stride), digit in zip(stages, digits):
        for j in range(1, r):
            peer = me + (partner(digit, j, r) - digit) * stride
            pl.semaphore_signal(barrier, inc=1, device_id=(peer,), device_id_type=MESH)
            peers += 1

    ctx = {"me": me, "digits": digits, "stages": stages, "sems": Semaphores(send, recv)}
    kept = up(iters, 4)
    unit = 2 * high // halves
    grams = [
        Stream(ctx, gram[g], kept * halves, unit, gheld[g], glanded[g]) for g in range(pieces)
    ]
    streams = [Stream(ctx, part[p], resp, high, held[p], landed[p]) for p in range(parts)]

    prepare(basis, iters, loads, chosen_ref, x_ref, res_ref, multi_ref, active_ref, twice, turned, rows)
    per = high * LANES // basis.stride
    hold = 1
    flying = []
    for p in range(parts):
        blocks = basis.blocks[p * per : (p + 1) * per]
        correlate(basis, blocks, deep, twice, turned, rows, acc)
        count = len(blocks) * basis.stride // LANES
        for b in range(count):
            t = acc[b * LANES : (b + 1) * LANES, :].T
            corr = t[0:resp] + t[resp : 2 * resp]
            for q in range(0, resp, 8):
                part[p][pl.ds(q * high + b, 8, stride=high), :] = corr[q : q + 8]
            gram[p // 2][pl.ds(p % 2 * high + b, 8, stride=2 * high), :] = t[2 * resp : 2 * resp + 8]
        if count < high:
            res = res_ref[...]
            sq = jnp.broadcast_to(jnp.sum(res * res, axis=1, keepdims=True), (resp, LANES))
            for b in range(count, high):
                for q in range(0, resp, 8):
                    part[p][pl.ds(q * high + b, 8, stride=high), :] = sq[q : q + 8]
                gram[p // 2][pl.ds(p % 2 * high + b, 8, stride=2 * high), :] = jnp.zeros(
                    (8, LANES), jnp.float32
                )
        if p < hold:
            continue
        if p == hold:
            pl.semaphore_wait(barrier, peers)
        sent, flying = flying, []
        for s in sent:
            s.receive(0)
            if k > 1:
                s.send(1)
        for i in range(p + 1) if p == hold else [p]:
            flying.append(streams[i])
            if i % 2:
                flying.append(grams[i // 2])
        for s in flying:
            s.send(0)

    line, lane = place(multi_ref[...], basis)
    maps[...] = jnp.zeros_like(maps)
    maps[0:1, 0:cands] = line
    maps[1:2, 0:cands] = lane
    def advance(s, stage):
        s.receive(stage)
        if stage + 1 < k:
            s.send(stage + 1)

    order = []
    for p in range(parts):
        order.append(streams[p])
        if p % 2:
            order.append(grams[p // 2])
    early = order[: len(order) // 2] if k > 1 else []
    for s in early:
        advance(s, 1)
    for s in flying:
        advance(s, 0)
    for c in range(0, maps.shape[1], LANES):
        at = maps[0:1, c : c + LANES]
        row = lax.broadcasted_iota(jnp.int32, (height, LANES), 0).astype(jnp.float32)
        one = jnp.where(row == at, 1.0, 0.0).astype(jnp.bfloat16)
        for i in range(3):
            hot[i * height : (i + 1) * height, c : c + LANES] = one
    for stage in range(1, k):
        for s in order:
            if stage > 1 or s not in early:
                advance(s, stage)

    gplan, plan = grams[0].plan, streams[0].plan
    at = pl.multiple_of(digit_place(ctx, gplan, digits) * unit, 8)
    runs = []
    for g in range(pieces):
        whole_gram[g][pl.ds(at, gplan[-1][1] * unit), :] = grams[g].now[...]
        runs.append(spread(ctx, gplan, unit, unit, whole_gram[g]))

    def arrange(row, store):
        first, rest = split(row)
        _, third = split(row - first.astype(jnp.float32))
        stacked = jnp.concatenate([first, rest, third], axis=0)
        wide = 4 * LANES
        for c in range(0, maps.shape[1], wide):
            size = min(wide, maps.shape[1] - c)
            found = lax.dot_general(
                stacked, hot[:, c : c + size], TN, preferred_element_type=jnp.float32
            )
            for i in range(0, size, LANES):
                at = maps[1:2, c + i : c + i + LANES]
                lo = lax.broadcasted_iota(jnp.int32, (LANES, LANES), 0).astype(jnp.float32)
                kept = jnp.where(lo == at, found[:, i : i + LANES], 0.0)
                store((c + i) // LANES, jnp.sum(kept, axis=0, keepdims=True))

    mine = digit_place(ctx, plan, digits) * height

    def arranged(row):
        found = {}
        arrange(row, found.__setitem__)
        lines = [row[height - 1 :]] * (height - len(found))
        return jnp.concatenate([found[b] for b in range(len(found))] + lines, axis=0)

    for i in range(plan[-1][1]):
        row = jnp.concatenate([s.now[i * high : (i + 1) * high, :] for s in streams], axis=0)
        total[pl.ds(pl.multiple_of(mine + i * height, 8), height), :] = arranged(row)
    run = spread(ctx, plan, height, up(maps.shape[1] // LANES + 1, tile), total)
    last = [s for s, (cut, _) in enumerate(plan) if cut][-1]
    todo = list(range(iters))

    def gram_row():
        if len(todo) == iters:
            for r in runs:
                for _ in r:
                    pass
        g = todo.pop(0)
        span = slice(g * 2 * high, (g + 1) * 2 * high)
        row = jnp.concatenate([w[span, :] for w in whole_gram], axis=0)
        out_ref[(resp + g) * height : (resp + g + 1) * height, :] = arranged(row)

    since = 0
    for level in run:
        if level == last:
            continue
        since += 1
        if todo and since % 3 == 0:
            gram_row()
    while todo:
        gram_row()
    rest = out_ref.shape[0] - (resp + iters) * height
    out_ref[(resp + iters) * height :, :] = jnp.zeros((rest, LANES), jnp.float32)
    out_ref[0 : resp * height, :] = total[...]
    for c in ctx["sems"].sent:
        c.wait_send()


def finish(cands, samples, iters, height, chosen_ref, total_ref, res_ref, active_ref, out_ref, corr_out, coef_ref, flat, corr_ref, sems):
    resp = res_ref.shape[0]
    for b in range(flat.shape[1] // LANES):
        for q in range(0, flat.shape[0], 8):
            flat[q : q + 8, b * LANES : (b + 1) * LANES] = total_ref[
                pl.ds(q * height + b, 8, stride=height), :
            ]
    sq = jnp.concatenate(
        [
            total_ref[pl.ds(q * height + flat.shape[1] // LANES, 8, stride=height), :]
            for q in range(0, resp, 8)
        ],
        axis=0,
    )[:, 0:1]
    total = flat[:, 0:cands]
    column = lax.broadcasted_iota(jnp.int32, total.shape, 1)
    picked = [
        jnp.sum(jnp.where(column == chosen_ref[i], total, 0.0), axis=1, keepdims=True)
        for i in range(iters)
    ]
    target = [p[0:resp] for p in picked]
    gram = [[picked[j][resp + i : resp + i + 1] for j in range(iters)] for i in range(iters)]
    tri = [[None] * iters for _ in range(iters)]
    for i in range(iters):
        for j in range(i + 1):
            s = gram[i][j]
            for m in range(j):
                s = s - tri[i][m] * tri[j][m]
            tri[i][j] = jnp.sqrt(s) if i == j else s / tri[j][j]
    corr = total[0:resp]
    rows = [total[resp + i : resp + i + 1] for i in range(iters)]
    coef = [jnp.zeros((resp, 1), jnp.float32) for _ in range(iters)]
    copies = []
    for k in range(iters):
        norm = math.sqrt(samples) * jnp.sqrt(sq / samples + 1e-06)
        corr_ref[k] = corr * (1.0 / norm)
        copies.append(pltpu.make_async_copy(corr_ref.at[k], corr_out.at[k], sems.at[k]))
        copies[-1].start()
        largest = jnp.max(jnp.abs(corr), axis=1, keepdims=True)
        gamma = jnp.abs(target[k]) / (largest + 1e-06)
        w = []
        for i in range(k + 1):
            s = target[i]
            for m in range(i):
                s = s - tri[i][m] * w[m]
            w.append(s / tri[i][i])
        for i in reversed(range(k + 1)):
            s = w[i]
            for m in range(i + 1, k + 1):
                s = s - tri[m][i] * w[m]
            w[i] = s / tri[i][i]
        step = [gamma * wi for wi in w]
        for i in range(k + 1):
            coef[i] = coef[i] + step[i]
        if k < iters - 1:
            gain = sum(wi * t for wi, t in zip(w, target))
            sq = jnp.maximum(sq - gamma * (2.0 - gamma) * gain, 0.0)
            target = [
                target[j] - sum(step[i] * gram[i][j] for i in range(k + 1)) for j in range(iters)
            ]
            for i in range(k + 1):
                corr = corr - step[i] * rows[i]
    res = res_ref[...]
    active = active_ref[...].astype(jnp.float32)
    for i in range(iters):
        res = res - coef[i] * active[i : i + 1]
    out_ref[...] = res
    shape = (resp, resp)
    eye = lax.broadcasted_iota(jnp.int32, shape, 0) == lax.broadcasted_iota(jnp.int32, shape, 1)
    lines = [jnp.sum(jnp.where(eye, c, 0.0), axis=0, keepdims=True) for c in coef]
    line = lax.broadcasted_iota(jnp.int32, coef_ref.shape, 0)
    coef_ref[...] = sum(jnp.where(line == i, lines[i], 0.0) for i in range(iters))
    for c in copies:
        c.wait()


def on_device(inputs, response, multi_index, chosen):
    nvars, width = inputs.shape
    devices = lax.axis_size("samp")
    samples = width * devices
    cands = multi_index.shape[0]
    iters = chosen.shape[0]
    resp = response.shape[0]
    basis = Basis(nvars)
    height, stride = basis.height, basis.stride
    few = up(iters, 16)
    kept = up(iters, 4)
    extra = up(kept, 8)
    used = resp + extra
    multi = multi_index.T
    vmem = pl.BlockSpec(memory_space=pltpu.VMEM)
    smem = pl.BlockSpec(memory_space=pltpu.SMEM)
    hbm = pl.BlockSpec(memory_space=pltpu.HBM)
    deep = width
    halves, parts, tile = 2, 6, 4
    high = height // parts
    unit, pieces = 2 * high // halves, parts // 2
    stages = radices(devices)
    plan, gplan = halving(resp, stages), halving(kept * halves, stages)
    copies = (parts + pieces) * sum(r - 1 for r, _ in stages)
    copies += resp // plan[-1][1] - 1 + pieces * (kept * halves // gplan[-1][1] - 1)
    grid = up(cands, LANES)
    lines = lambda n: pltpu.VMEM((n, LANES), jnp.float32)
    held = [lines(c * high) for _, c in plan]
    landed = [lines(r * c * high) for (r, _), (_, c) in zip(stages, plan)]
    gheld = [lines(c * unit) for _, c in gplan]
    glanded = [lines(r * c * unit) for (r, _), (_, c) in zip(stages, gplan)]
    total, active = pl.pallas_call(
        functools.partial(learn, basis, devices, parts, iters, deep, halves, tile),
        in_specs=[smem, hbm, hbm, hbm],
        out_specs=[vmem, vmem],
        out_shape=[
            jax.ShapeDtypeStruct((used * height, LANES), jnp.float32),
            jax.ShapeDtypeStruct((few, width), jnp.bfloat16),
        ],
        scratch_shapes=[
            pltpu.SemaphoreType.DMA((copies,)),
            pltpu.SemaphoreType.DMA((copies,)),
            pltpu.SemaphoreType.DMA((3,)),
            pltpu.VMEM(inputs.shape, jnp.float32),
            pltpu.VMEM(response.shape, jnp.float32),
            pltpu.VMEM(multi.shape, jnp.int32),
            pltpu.VMEM((3 * stride, width), jnp.float32),
            pltpu.VMEM((2 * nvars * stride, width), jnp.float32),
            pltpu.VMEM((up(2 * resp + few, LANES), width), jnp.bfloat16),
            lines(high * LANES),
            lines(resp * height),
            pltpu.VMEM((8, grid), jnp.float32),
            pltpu.VMEM((3 * height, grid), jnp.bfloat16),
            *[lines(resp * high) for _ in range(parts)],
            *(held * parts),
            *(landed * parts),
            *[lines(up(kept, 8) * 2 * high) for _ in range(pieces)],
            *[lines(kept * 2 * high) for _ in range(pieces)],
            *(gheld * pieces),
            *(glanded * pieces),
        ],
        compiler_params=pltpu.CompilerParams(
            vmem_limit_bytes=VMEM_LIMIT, collective_id=0, has_side_effects=True
        ),
        name="learn",
    )(chosen, inputs, response, multi)
    residual, corr, coef = pl.pallas_call(
        functools.partial(finish, cands, samples, iters, height),
        in_specs=[smem, vmem, vmem, vmem],
        out_specs=[vmem, pl.BlockSpec(memory_space=pl.ANY), vmem],
        out_shape=[
            jax.ShapeDtypeStruct((resp, width), jnp.float32),
            jax.ShapeDtypeStruct((iters, resp, cands), jnp.float32),
            jax.ShapeDtypeStruct((iters, resp), jnp.float32),
        ],
        scratch_shapes=[
            pltpu.VMEM((used, grid), jnp.float32),
            pltpu.VMEM((iters, resp, cands), jnp.float32),
            pltpu.SemaphoreType.DMA((iters,)),
        ],
        compiler_params=pltpu.CompilerParams(vmem_limit_bytes=VMEM_LIMIT),
        name="finish",
    )(chosen, total, response, active)
    return residual, corr, coef


def solution(mesh):
    placed = (P(None, "samp"), P(None, "samp"), P(), P())
    return jax.shard_map(
        on_device,
        mesh=mesh,
        in_specs=placed,
        out_specs=(P(None, "samp"), P(), P()),
        check_vma=False,
    )
```

```python
import functools
import math

import jax
import jax.numpy as jnp
from jax import lax
from jax.experimental import pallas as pl
from jax.experimental.pallas import tpu as pltpu
from jax.sharding import PartitionSpec as P

LANES = 128
NT = (((1,), (1,)), ((), ()))
TN = (((0,), (0,)), ((), ()))
MESH = pl.DeviceIdType.MESH
VMEM_LIMIT = 57 * 2**20


def up(n, m):
    return -(-n // m) * m


def split(x):
    high = x.astype(jnp.bfloat16)
    return high, (x - high.astype(jnp.float32)).astype(jnp.bfloat16)


class Basis:
    def __init__(self, nvars):
        self.nvars = nvars
        self.stride = up(nvars + 1, 16)
        gaps = []
        d = 1
        while nvars - 3 * d > 0:
            gaps += [(d, e) for e in range(d, nvars - 2 * d)]
            d += 1
        if nvars % 3 == 0:
            gaps.append((nvars // 3, nvars // 3))
        self.triples = len(gaps)
        self.pairs = nvars // 2
        self.squares = nvars - 1
        self.blocks = [("triple", d, d + e) for d, e in gaps]
        self.blocks += [("pair", d, 0) for d in range(1, self.pairs + 1)]
        self.blocks += [("square", d, 0) for d in range(1, self.squares + 1)]
        self.blocks += [("single", e, 0) for e in range(3)]
        while len(self.blocks) * self.stride % LANES:
            self.blocks.append(("single", 0, 0))
        self.lines = len(self.blocks) * self.stride // LANES
        self.height = up(self.lines + 1, 48)


def place(multi, basis):
    n = float(basis.nvars)
    deg = multi.astype(jnp.float32)
    var = lax.broadcasted_iota(jnp.int32, multi.shape, 0).astype(jnp.float32)
    pos = deg > 0.0
    down = lambda f, x: f(x, axis=0, keepdims=True)
    count = down(jnp.sum, jnp.where(pos, 1.0, 0.0))
    total = down(jnp.sum, jnp.where(pos, var, 0.0))
    low = down(jnp.min, jnp.where(pos, var, n))
    high = down(jnp.max, jnp.where(pos, var, 0.0))
    most = down(jnp.max, deg)
    two = down(jnp.sum, jnp.where(deg > 1.5, var, 0.0))
    mid = total - low - high
    g1, g2 = mid - low, high - mid
    g3 = n - g1 - g2
    at_mid = jnp.logical_and(g2 <= g3, g2 < g1)
    at_high = jnp.logical_and(g3 <= g1, g3 < g2)
    pick = lambda a, b, c: jnp.where(at_high, c, jnp.where(at_mid, b, a))
    d1, d2, start3 = pick(g1, g2, g3), pick(g2, g3, g1), pick(low, mid, high)
    block3 = n * (d1 - 1.0) - 1.5 * d1 * (d1 - 1.0) + d2 - d1
    gap = high - low
    near = gap <= n - gap
    block2 = float(basis.triples - 1) + jnp.where(near, gap, n - gap)
    start2 = jnp.where(near, low, high)
    one = total - two
    turn = two - one
    block21 = float(basis.triples + basis.pairs - 1) + jnp.where(turn > 0.0, turn, turn + n)
    base = float(basis.triples + basis.pairs + basis.squares)
    block1 = base + jnp.maximum(most - 1.0, 0.0)
    squared = most > 1.5
    block = jnp.where(
        count > 2.5, block3, jnp.where(count > 1.5, jnp.where(squared, block21, block2), block1)
    )
    start = jnp.where(
        count > 2.5, start3, jnp.where(count > 1.5, jnp.where(squared, one, start2), low)
    )
    index = block * float(basis.stride) + start
    line = jnp.floor(index * (1.0 / LANES))
    return line, index - line * float(LANES)


def prepare(basis, iters, loads, chosen_ref, x_ref, res_ref, multi_ref, active_ref, twice, turned, rows):
    nvars, width = x_ref.shape
    resp = res_ref.shape[0]
    stride = basis.stride
    few = active_ref.shape[0]
    loads[0].wait()
    x = x_ref[...]
    second = (3.0 * x * x - 1.0) * 0.5
    third = (5.0 * x * x * x - 3.0 * x) * 0.5
    values = [x * math.sqrt(3.0), second * math.sqrt(5.0), third * math.sqrt(7.0)]
    for e, value in enumerate(values):
        twice[e * stride + nvars : (e + 1) * stride, :] = jnp.ones((stride - nvars, width), jnp.float32)
        twice[e * stride : e * stride + nvars, :] = value
    zero = jnp.zeros((stride - nvars, width), jnp.float32)
    for e in range(2):
        for d in range(1, nvars):
            at = (e * nvars + d) * stride
            turned[at : at + nvars - d, :] = values[e][d:]
            turned[at + nvars - d : at + nvars, :] = values[e][:d]
            turned[at + nvars : at + stride, :] = zero

    loads[1].wait()
    loads[2].wait()
    high, low = split(res_ref[...])
    rows[0:resp, :] = high
    rows[resp : 2 * resp, :] = low
    multi = multi_ref[...]
    column = lax.broadcasted_iota(jnp.int32, multi.shape, 1)
    line = lax.broadcasted_iota(jnp.int32, (few, width), 0)
    actives = jnp.zeros((few, width), jnp.float32)
    for k in range(iters):
        deg = jnp.sum(
            jnp.where(column == chosen_ref[k], multi, 0).astype(jnp.float32), axis=1, keepdims=True
        )
        v = jnp.where(
            deg > 2.5,
            values[2],
            jnp.where(deg > 1.5, values[1], jnp.where(deg > 0.5, values[0], 1.0)),
        )
        p = v[0:8]
        for i in range(8, nvars - 7, 8):
            p = p * v[i : i + 8]
        row = p[0:1]
        for i in range(1, min(8, nvars)):
            row = row * p[i : i + 1]
        for i in range(nvars // 8 * 8, nvars):
            row = row * v[i : i + 1]
        actives = jnp.where(line == k, row, actives)
    actives = actives.astype(jnp.bfloat16)
    active_ref[...] = actives
    rows[2 * resp : 2 * resp + few, :] = actives
    rest = rows.shape[0] - 2 * resp - few
    rows[2 * resp + few :, :] = jnp.zeros((rest, width), jnp.bfloat16)


def correlate(basis, blocks, deep, twice, turned, rows, acc):
    stride, nvars = basis.stride, basis.nvars
    width = rows.shape[1]
    per = 512 // stride
    groups = [blocks[i : i + per] for i in range(0, len(blocks), per)]

    def step(k, first):
        for g, group in enumerate(groups):
            total = None
            for half in range(0, deep, 256):
                at = k * deep + half
                cols = pl.ds(at if first else pl.multiple_of(at, 256), 256)
                f1 = twice[0:stride, cols]
                parts = []
                held = None
                for kind, d, e in group:
                    if kind == "triple":
                        if held != d:
                            pair = f1 * turned[d * stride : (d + 1) * stride, cols]
                            held = d
                        part = pair * turned[e * stride : (e + 1) * stride, cols]
                    elif kind == "pair":
                        part = f1 * turned[d * stride : (d + 1) * stride, cols]
                    elif kind == "square":
                        part = f1 * turned[(nvars + d) * stride : (nvars + d + 1) * stride, cols]
                    else:
                        part = twice[d * stride : (d + 1) * stride, cols]
                    parts.append(part.astype(jnp.bfloat16))
                psi = jnp.concatenate(parts, axis=0)
                term = lax.dot_general(psi, rows[:, cols], NT, preferred_element_type=jnp.float32)
                total = term if total is None else total + term
            span = slice(g * per * stride, (g * per + len(group)) * stride)
            acc[span, :] = total if first else acc[span, :] + total

    step(0, True)

    if width > deep:

        @pl.loop(1, width // deep)
        def _(k):
            step(k, False)


def radices(n):
    result, stride = [], 1
    while n > 1:
        r = 2 if stride == 1 or n == 2 else 4
        if n % r:
            raise ValueError("device count")
        result.append((r, stride))
        stride *= r
        n //= r
    return result


def partner(digit, j, r):
    result, bit = 0, 1
    while bit < r:
        b = lax.rem(digit // bit, 2)
        result = result + bit * (1 - b if j & bit else b)
        bit *= 2
    return result


def halving(count, stages):
    plan = []
    for r, _ in stages:
        cut = count % r == 0
        count = count // r if cut else count
        plan.append((cut, count))
    return plan


class Semaphores:
    def __init__(self, send, recv):
        self.send, self.recv, self.used, self.sent = send, recv, 0, []

    def copy(self, src, dst, peer):
        c = pltpu.make_async_remote_copy(
            src_ref=src,
            dst_ref=dst,
            send_sem=self.send.at[self.used],
            recv_sem=self.recv.at[self.used],
            device_id=(peer,),
            device_id_type=MESH,
        )
        self.used += 1
        self.sent.append(c)
        c.start()
        return c


class Stream:
    def __init__(self, ctx, part, count, unit, held, landed):
        self.ctx, self.unit = ctx, unit
        self.now = part
        self.held, self.landed = held, landed
        self.plan = halving(count, ctx["stages"])
        self.waiting = None

    def send(self, s):
        r, stride = self.ctx["stages"][s]
        digit = self.ctx["digits"][s]
        cut, count = self.plan[s]
        size = count * self.unit
        copies = []
        for j in range(r - 1, 0, -1):
            other = partner(digit, j, r)
            peer = self.ctx["me"] + (other - digit) * stride
            at = pl.multiple_of(other * size, 8) if cut else 0
            copies.append(
                self.ctx["sems"].copy(
                    self.now.at[pl.ds(at, size)], self.landed[s].at[pl.ds(j * size, size)], peer
                )
            )
        self.waiting = copies

    def receive(self, s):
        r, _ = self.ctx["stages"][s]
        digit = self.ctx["digits"][s]
        cut, count = self.plan[s]
        size = count * self.unit
        for c in self.waiting:
            c.wait_recv()
        at = pl.multiple_of(digit * size, 8) if cut else 0
        own = self.now[pl.ds(at, size), :]
        landed = self.landed[s]
        if cut:
            total = own
            for j in range(1, r):
                total = total + landed[j * size : (j + 1) * size, :]
        else:
            landed[0:size, :] = own
            total = None
            for i in range(r):
                at = pl.multiple_of(partner(digit, i, r) * size, 8)
                term = landed[pl.ds(at, size), :]
                total = term if total is None else total + term
        self.held[s][...] = total
        self.now = self.held[s]


def digit_place(ctx, plan, digits):
    at, weight = 0, plan[-1][1]
    for s in reversed(range(len(plan))):
        if plan[s][0]:
            at = at + digits[s] * weight
            weight *= ctx["stages"][s][0]
    return at


def spread(ctx, plan, unit, tall, whole):
    levels = [s for s, (cut, _) in enumerate(plan) if cut]
    size = (plan[-1][1] - 1) * unit + tall
    arriving = {s: [] for s in levels}

    def forward(digits, below):
        at = pl.multiple_of(digit_place(ctx, plan, digits) * unit, 8)
        block = whole.at[pl.ds(at, size)]
        for s in reversed(below):
            r, stride = ctx["stages"][s]
            digit = ctx["digits"][s]
            arrivals = []
            for j in range(r - 1, 0, -1):
                peer = ctx["me"] + (partner(digit, j, r) - digit) * stride
                c = ctx["sems"].copy(block, block, peer)
                source = dict(digits)
                source[s] = partner(digit, j, r)
                arrivals.insert(0, (c, source))
            arriving[s] += arrivals

    forward(dict(enumerate(ctx["digits"])), levels)

    def run():
        for i in reversed(range(len(levels))):
            for c, digits in arriving[levels[i]]:
                c.wait_recv()
                forward(digits, levels[:i])
                yield levels[i], digits

    return run()


def learn(basis, devices, parts, iters, deep, halves, tile, chosen_ref, x_in, res_in, multi_in, out_ref, active_ref, *scratch):
    scratch = list(scratch)
    resp, height = res_in.shape[0], basis.height
    high = height // parts
    cands = multi_in.shape[1]
    stages = radices(devices)
    me = lax.axis_index("samp")
    digits = [lax.rem(me // stride, r) for r, stride in stages]
    send, recv, loaded, stored, extra, x_ref, res_ref, multi_ref, twice, turned, rows, acc, total, maps, hot = scratch[:15]
    buffers = scratch[15:]
    loads = []
    for i, (a, b) in enumerate([(x_in, x_ref), (multi_in, multi_ref), (res_in, res_ref)]):
        loads.append(pltpu.make_async_copy(a, b, loaded.at[i]))
        loads[-1].start()
    k = len(stages)
    take = lambda n: [buffers.pop(0) for _ in range(n)]
    part = take(parts)
    held = [take(k) for _ in range(parts)]
    landed = [take(k) for _ in range(parts)]
    pieces = parts // 2
    gram, whole_gram = take(pieces), take(pieces)
    gheld = [take(k) for _ in range(pieces)]
    glanded = [take(k) for _ in range(pieces)]

    barrier = pltpu.get_barrier_semaphore()
    peers = 0
    for (r, stride), digit in zip(stages, digits):
        for j in range(1, r):
            peer = me + (partner(digit, j, r) - digit) * stride
            pl.semaphore_signal(barrier, inc=1, device_id=(peer,), device_id_type=MESH)
            peers += 1

    ctx = {"me": me, "digits": digits, "stages": stages, "sems": Semaphores(send, recv)}
    kept = up(iters, 4)
    unit = 2 * high // halves
    grams = [
        Stream(ctx, gram[g], kept * halves, unit, gheld[g], glanded[g]) for g in range(pieces)
    ]
    streams = [Stream(ctx, part[p], resp, high, held[p], landed[p]) for p in range(parts)]

    prepare(basis, iters, loads, chosen_ref, x_ref, res_ref, multi_ref, active_ref, twice, turned, rows)
    per = high * LANES // basis.stride
    hold = 1
    flying = []
    for p in range(parts):
        blocks = basis.blocks[p * per : (p + 1) * per]
        correlate(basis, blocks, deep, twice, turned, rows, acc)
        count = len(blocks) * basis.stride // LANES
        for b in range(count):
            t = acc[b * LANES : (b + 1) * LANES, :].T
            corr = t[0:resp] + t[resp : 2 * resp]
            for q in range(0, resp, 8):
                part[p][pl.ds(q * high + b, 8, stride=high), :] = corr[q : q + 8]
            gram[p // 2][pl.ds(p % 2 * high + b, 8, stride=2 * high), :] = t[2 * resp : 2 * resp + 8]
        if count < high:
            res = res_ref[...]
            sq = jnp.broadcast_to(jnp.sum(res * res, axis=1, keepdims=True), (resp, LANES))
            for b in range(count, high):
                for q in range(0, resp, 8):
                    part[p][pl.ds(q * high + b, 8, stride=high), :] = sq[q : q + 8]
                gram[p // 2][pl.ds(p % 2 * high + b, 8, stride=2 * high), :] = jnp.zeros(
                    (8, LANES), jnp.float32
                )
        if p < hold:
            continue
        if p == hold:
            pl.semaphore_wait(barrier, peers)
        sent, flying = flying, []
        for s in sent:
            s.receive(0)
            if k > 1:
                s.send(1)
        for i in range(p + 1) if p == hold else [p]:
            flying.append(streams[i])
            if i % 2:
                flying.append(grams[i // 2])
        for s in flying:
            s.send(0)

    line, lane = place(multi_ref[...], basis)
    maps[...] = jnp.zeros_like(maps)
    maps[0:1, 0:cands] = line
    maps[1:2, 0:cands] = lane
    def advance(s, stage):
        s.receive(stage)
        if stage + 1 < k:
            s.send(stage + 1)

    order = []
    for p in range(parts):
        order.append(streams[p])
        if p % 2:
            order.append(grams[p // 2])
    early = order[: len(order) // 2] if k > 1 else []
    for s in early:
        advance(s, 1)
    for s in flying:
        advance(s, 0)
    for c in range(0, maps.shape[1], LANES):
        at = maps[0:1, c : c + LANES]
        row = lax.broadcasted_iota(jnp.int32, (height, LANES), 0).astype(jnp.float32)
        one = jnp.where(row == at, 1.0, 0.0).astype(jnp.bfloat16)
        for i in range(3):
            hot[i * height : (i + 1) * height, c : c + LANES] = one
    for stage in range(1, k):
        for s in order:
            if stage > 1 or s not in early:
                advance(s, stage)

    gplan, plan = grams[0].plan, streams[0].plan
    at = pl.multiple_of(digit_place(ctx, gplan, digits) * unit, 8)
    runs = []
    for g in range(pieces):
        whole_gram[g][pl.ds(at, gplan[-1][1] * unit), :] = grams[g].now[...]
        runs.append(spread(ctx, gplan, unit, unit, whole_gram[g]))

    def arrange(row, store):
        first, rest = split(row)
        _, third = split(row - first.astype(jnp.float32))
        stacked = jnp.concatenate([first, rest, third], axis=0)
        wide = 4 * LANES
        for c in range(0, maps.shape[1], wide):
            size = min(wide, maps.shape[1] - c)
            found = lax.dot_general(
                stacked, hot[:, c : c + size], TN, preferred_element_type=jnp.float32
            )
            for i in range(0, size, LANES):
                at = maps[1:2, c + i : c + i + LANES]
                lo = lax.broadcasted_iota(jnp.int32, (LANES, LANES), 0).astype(jnp.float32)
                kept = jnp.where(lo == at, found[:, i : i + LANES], 0.0)
                store((c + i) // LANES, jnp.sum(kept, axis=0, keepdims=True))

    mine = digit_place(ctx, plan, digits) * height

    def arranged(row):
        found = {}
        arrange(row, found.__setitem__)
        lines = [row[height - 1 :]] * (height - len(found))
        return jnp.concatenate([found[b] for b in range(len(found))] + lines, axis=0)

    for i in range(plan[-1][1]):
        row = jnp.concatenate([s.now[i * high : (i + 1) * high, :] for s in streams], axis=0)
        total[pl.ds(pl.multiple_of(mine + i * height, 8), height), :] = arranged(row)
    run = spread(ctx, plan, height, up(maps.shape[1] // LANES + 1, tile), total)
    last = [s for s, (cut, _) in enumerate(plan) if cut][-1]
    size = (plan[-1][1] - 1) * height + up(maps.shape[1] // LANES + 1, tile)
    stores = []

    def store(src, dst):
        stores.append(pltpu.make_async_copy(src, dst, stored.at[len(stores)]))
        stores[-1].start()

    def keep(source):
        at = pl.multiple_of(digit_place(ctx, plan, source) * height, 8)
        store(total.at[pl.ds(at, size)], out_ref.at[pl.ds(at, size)])

    keep(dict(enumerate(digits)))
    rest = extra.shape[0] - iters * height
    extra[iters * height :, :] = jnp.zeros((rest, LANES), jnp.float32)
    store(
        extra.at[pl.ds(iters * height, rest)],
        out_ref.at[pl.ds((resp + iters) * height, rest)],
    )
    todo = list(range(iters))

    def gram_row():
        if len(todo) == iters:
            for r in runs:
                for _ in r:
                    pass
        g = todo.pop(0)
        span = slice(g * 2 * high, (g + 1) * 2 * high)
        row = jnp.concatenate([w[span, :] for w in whole_gram], axis=0)
        extra[g * height : (g + 1) * height, :] = arranged(row)
        store(
            extra.at[pl.ds(g * height, height)],
            out_ref.at[pl.ds((resp + g) * height, height)],
        )

    since = 0
    for level, source in run:
        keep(source)
        if level == last:
            continue
        since += 1
        if todo and since % 3 == 0:
            gram_row()
    while todo:
        gram_row()
    for c in stores:
        c.wait()
    for c in ctx["sems"].sent:
        c.wait_send()


def finish(cands, samples, iters, height, chosen_ref, total_ref, res_ref, active_ref, out_ref, corr_out, coef_ref, flat, corr_ref, sems):
    resp = res_ref.shape[0]
    for b in range(flat.shape[1] // LANES):
        for q in range(0, flat.shape[0], 8):
            flat[q : q + 8, b * LANES : (b + 1) * LANES] = total_ref[
                pl.ds(q * height + b, 8, stride=height), :
            ]
    sq = jnp.concatenate(
        [
            total_ref[pl.ds(q * height + flat.shape[1] // LANES, 8, stride=height), :]
            for q in range(0, resp, 8)
        ],
        axis=0,
    )[:, 0:1]
    total = flat[:, 0:cands]
    column = lax.broadcasted_iota(jnp.int32, total.shape, 1)
    picked = [
        jnp.sum(jnp.where(column == chosen_ref[i], total, 0.0), axis=1, keepdims=True)
        for i in range(iters)
    ]
    target = [p[0:resp] for p in picked]
    gram = [[picked[j][resp + i : resp + i + 1] for j in range(iters)] for i in range(iters)]
    tri = [[None] * iters for _ in range(iters)]
    for i in range(iters):
        for j in range(i + 1):
            s = gram[i][j]
            for m in range(j):
                s = s - tri[i][m] * tri[j][m]
            tri[i][j] = jnp.sqrt(s) if i == j else s / tri[j][j]
    corr = total[0:resp]
    rows = [total[resp + i : resp + i + 1] for i in range(iters)]
    coef = [jnp.zeros((resp, 1), jnp.float32) for _ in range(iters)]
    copies = []
    for k in range(iters):
        norm = math.sqrt(samples) * jnp.sqrt(sq / samples + 1e-06)
        corr_ref[k] = corr * (1.0 / norm)
        copies.append(pltpu.make_async_copy(corr_ref.at[k], corr_out.at[k], sems.at[k]))
        copies[-1].start()
        largest = jnp.max(jnp.abs(corr), axis=1, keepdims=True)
        gamma = jnp.abs(target[k]) / (largest + 1e-06)
        w = []
        for i in range(k + 1):
            s = target[i]
            for m in range(i):
                s = s - tri[i][m] * w[m]
            w.append(s / tri[i][i])
        for i in reversed(range(k + 1)):
            s = w[i]
            for m in range(i + 1, k + 1):
                s = s - tri[m][i] * w[m]
            w[i] = s / tri[i][i]
        step = [gamma * wi for wi in w]
        for i in range(k + 1):
            coef[i] = coef[i] + step[i]
        if k < iters - 1:
            gain = sum(wi * t for wi, t in zip(w, target))
            sq = jnp.maximum(sq - gamma * (2.0 - gamma) * gain, 0.0)
            target = [
                target[j] - sum(step[i] * gram[i][j] for i in range(k + 1)) for j in range(iters)
            ]
            for i in range(k + 1):
                corr = corr - step[i] * rows[i]
    res = res_ref[...]
    active = active_ref[...].astype(jnp.float32)
    for i in range(iters):
        res = res - coef[i] * active[i : i + 1]
    out_ref[...] = res
    shape = (resp, resp)
    eye = lax.broadcasted_iota(jnp.int32, shape, 0) == lax.broadcasted_iota(jnp.int32, shape, 1)
    lines = [jnp.sum(jnp.where(eye, c, 0.0), axis=0, keepdims=True) for c in coef]
    line = lax.broadcasted_iota(jnp.int32, coef_ref.shape, 0)
    coef_ref[...] = sum(jnp.where(line == i, lines[i], 0.0) for i in range(iters))
    for c in copies:
        c.wait()


def on_device(inputs, response, multi_index, chosen):
    nvars, width = inputs.shape
    devices = lax.axis_size("samp")
    samples = width * devices
    cands = multi_index.shape[0]
    iters = chosen.shape[0]
    resp = response.shape[0]
    basis = Basis(nvars)
    height, stride = basis.height, basis.stride
    few = up(iters, 16)
    kept = up(iters, 4)
    extra = up(kept, 8)
    used = resp + extra
    multi = multi_index.T
    vmem = pl.BlockSpec(memory_space=pltpu.VMEM)
    smem = pl.BlockSpec(memory_space=pltpu.SMEM)
    hbm = pl.BlockSpec(memory_space=pltpu.HBM)
    deep = width
    halves, parts, tile = 2, 6, 4
    high = height // parts
    unit, pieces = 2 * high // halves, parts // 2
    stages = radices(devices)
    plan, gplan = halving(resp, stages), halving(kept * halves, stages)
    copies = (parts + pieces) * sum(r - 1 for r, _ in stages)
    copies += resp // plan[-1][1] - 1 + pieces * (kept * halves // gplan[-1][1] - 1)
    grid = up(cands, LANES)
    lines = lambda n: pltpu.VMEM((n, LANES), jnp.float32)
    held = [lines(c * high) for _, c in plan]
    landed = [lines(r * c * high) for (r, _), (_, c) in zip(stages, plan)]
    gheld = [lines(c * unit) for _, c in gplan]
    glanded = [lines(r * c * unit) for (r, _), (_, c) in zip(stages, gplan)]
    total, active = pl.pallas_call(
        functools.partial(learn, basis, devices, parts, iters, deep, halves, tile),
        in_specs=[smem, hbm, hbm, hbm],
        out_specs=[hbm, vmem],
        out_shape=[
            jax.ShapeDtypeStruct((used * height, LANES), jnp.float32),
            jax.ShapeDtypeStruct((few, width), jnp.bfloat16),
        ],
        scratch_shapes=[
            pltpu.SemaphoreType.DMA((copies,)),
            pltpu.SemaphoreType.DMA((copies,)),
            pltpu.SemaphoreType.DMA((3,)),
            pltpu.SemaphoreType.DMA((resp // plan[-1][1] + iters + 1,)),
            lines(extra * height),
            pltpu.VMEM(inputs.shape, jnp.float32),
            pltpu.VMEM(response.shape, jnp.float32),
            pltpu.VMEM(multi.shape, jnp.int32),
            pltpu.VMEM((3 * stride, width), jnp.float32),
            pltpu.VMEM((2 * nvars * stride, width), jnp.float32),
            pltpu.VMEM((up(2 * resp + few, LANES), width), jnp.bfloat16),
            lines(high * LANES),
            lines(resp * height),
            pltpu.VMEM((8, grid), jnp.float32),
            pltpu.VMEM((3 * height, grid), jnp.bfloat16),
            *[lines(resp * high) for _ in range(parts)],
            *(held * parts),
            *(landed * parts),
            *[lines(up(kept, 8) * 2 * high) for _ in range(pieces)],
            *[lines(kept * 2 * high) for _ in range(pieces)],
            *(gheld * pieces),
            *(glanded * pieces),
        ],
        compiler_params=pltpu.CompilerParams(
            vmem_limit_bytes=VMEM_LIMIT, collective_id=0, has_side_effects=True
        ),
        name="learn",
    )(chosen, inputs, response, multi)
    residual, corr, coef = pl.pallas_call(
        functools.partial(finish, cands, samples, iters, height),
        in_specs=[smem, vmem, vmem, vmem],
        out_specs=[vmem, pl.BlockSpec(memory_space=pl.ANY), vmem],
        out_shape=[
            jax.ShapeDtypeStruct((resp, width), jnp.float32),
            jax.ShapeDtypeStruct((iters, resp, cands), jnp.float32),
            jax.ShapeDtypeStruct((iters, resp), jnp.float32),
        ],
        scratch_shapes=[
            pltpu.VMEM((used, grid), jnp.float32),
            pltpu.VMEM((iters, resp, cands), jnp.float32),
            pltpu.SemaphoreType.DMA((iters,)),
        ],
        compiler_params=pltpu.CompilerParams(vmem_limit_bytes=VMEM_LIMIT),
        name="finish",
    )(chosen, total, response, active)
    return residual, corr, coef


def solution(mesh):
    placed = (P(None, "samp"), P(None, "samp"), P(), P())
    return jax.shard_map(
        on_device,
        mesh=mesh,
        in_specs=placed,
        out_specs=(P(None, "samp"), P(), P()),
        check_vma=False,
    )
```
